16 devices in a mesh: fsdp: 16 (over z, y, x, core).
Axes of the slice: x: 2, y: 2, z: 2, core: 2. Of those that a mesh axis runs over, the one named last changes fastest.
Arguments:
- tokens: int32 [16, 1024], P('fsdp')
- labels: int32 [16, 1024], P('fsdp')
- loss_mask: int32 [16, 1024], P('fsdp')
- hidden: bfloat16 [16, 1024, 960], P('fsdp')
- d_emb: bfloat16 [16, 1024, 960], P('fsdp')
- embed_table: bfloat16 [49152, 960], P('fsdp')
- ln_gain: float32 [960], P('fsdp')
- ln_bias: float32 [960], P('fsdp')
Outputs:
- output 1: bfloat16 [16, 1024, 960], P('fsdp')
- output 2: float32 [], replicated
- output 3: bfloat16 [16, 1024, 960], P('fsdp')
- output 4: float32 [49152, 960], P('fsdp')
- output 5: float32 [960], P('fsdp')
- output 6: float32 [960], P('fsdp')
All inputs are finite; a program needn't handle non-finite values.
Results may differ from the reference program's by a relative error of at most 0.001.
Values are sent between devices in bfloat16 or wider.
A program may use at most 1 GiB of HBM per device.

```python
import jax
import jax.numpy as jnp
from jax import lax

VOCAB_SIZE = 49152
MODEL_DIM = 960
BATCH_ROWS = 16
SEQ_LEN = 1024
GROUP_SIZE = 16

LN_EPSILON = 1e-5
SHARD_ROWS = VOCAB_SIZE // GROUP_SIZE
ROWS_PER_DEV = BATCH_ROWS // GROUP_SIZE
TOKEN_TOTAL = BATCH_ROWS * SEQ_LEN


def draw_ids(id_key, id_shape):
    key_one, key_two, key_three = jax.random.split(id_key, 3)
    draw_one = jax.random.randint(key_one, id_shape, 0, VOCAB_SIZE, dtype=jnp.int32)
    draw_two = jax.random.randint(key_two, id_shape, 0, VOCAB_SIZE, dtype=jnp.int32)
    pick_kind = jax.random.randint(key_three, id_shape, 0, 4, dtype=jnp.int32)
    return jnp.where(pick_kind < 3, jnp.minimum(draw_one, draw_two), draw_one)


def draw_mask(mask_key):
    key_one, key_two = jax.random.split(mask_key)
    dev_cut = jax.random.randint(key_one, (GROUP_SIZE, 1), 0, SEQ_LEN // 2 + 1, dtype=jnp.int32)
    row_cut = jax.random.randint(key_two, (GROUP_SIZE, ROWS_PER_DEV), 0, SEQ_LEN // 4 + 1, dtype=jnp.int32)
    lengths = (SEQ_LEN - dev_cut - row_cut).reshape(BATCH_ROWS, 1)
    positions = jnp.arange(SEQ_LEN, dtype=jnp.int32)[None, :]
    return (positions < lengths).astype(jnp.int32)


def setup_inputs(seed: int = 0) -> dict:
    key_list = jax.random.split(jax.random.key(seed), 8)
    act_shape = (BATCH_ROWS, SEQ_LEN, MODEL_DIM)
    tokens = draw_ids(key_list[0], (BATCH_ROWS, SEQ_LEN))
    labels = draw_ids(key_list[1], (BATCH_ROWS, SEQ_LEN))
    loss_mask = draw_mask(key_list[2])
    hidden = jax.random.normal(key_list[3], act_shape, jnp.float32).astype(jnp.bfloat16)
    d_emb = (jax.random.normal(key_list[4], act_shape, jnp.float32) * (2.0 / TOKEN_TOTAL)).astype(jnp.bfloat16)
    embed_table = (jax.random.normal(key_list[5], (VOCAB_SIZE, MODEL_DIM), jnp.float32) * (2.0 * MODEL_DIM ** -0.5)).astype(jnp.bfloat16)
    ln_gain = 1.0 + 0.3 * jax.random.normal(key_list[6], (MODEL_DIM,), jnp.float32)
    ln_bias = 0.3 * jax.random.normal(key_list[7], (MODEL_DIM,), jnp.float32)
    return {'tokens': tokens, 'labels': labels, 'loss_mask': loss_mask, 'hidden': hidden, 'd_emb': d_emb, 'embed_table': embed_table, 'ln_gain': ln_gain, 'ln_bias': ln_bias}


def layer_norm(inputs, ln_gain, ln_bias):
    row_mean = jnp.mean(inputs, axis=-1, keepdims=True)
    centred = inputs - row_mean
    row_var = jnp.mean(centred * centred, axis=-1, keepdims=True)
    return centred * lax.rsqrt(row_var + LN_EPSILON) * ln_gain + ln_bias


def reference(tokens, labels, loss_mask, hidden, d_emb, embed_table, ln_gain, ln_bias):
    tok_flat = tokens.reshape(-1)
    label_flat = labels.reshape(-1)
    mask_flat = loss_mask.reshape(-1).astype(jnp.float32)
    weight = mask_flat / jnp.sum(mask_flat)
    emb_rows = jnp.take(embed_table, tok_flat, axis=0).reshape(BATCH_ROWS, SEQ_LEN, MODEL_DIM)
    normed, ln_vjp = jax.vjp(layer_norm, hidden.reshape(-1, MODEL_DIM).astype(jnp.float32), ln_gain, ln_bias)
    normed_bf = normed.astype(jnp.bfloat16)
    vocab_blocks = embed_table.reshape(GROUP_SIZE, SHARD_ROWS, MODEL_DIM)
    block_starts = jnp.arange(GROUP_SIZE, dtype=jnp.int32) * SHARD_ROWS
    col_offsets = jnp.arange(SHARD_ROWS, dtype=jnp.int32)

    def max_step(scan_carry, vocab_block):
        run_max, run_sum = scan_carry
        logits = jnp.dot(normed_bf, vocab_block.T, preferred_element_type=jnp.float32)
        new_max = jnp.maximum(run_max, jnp.max(logits, axis=1))
        run_sum = run_sum * jnp.exp(run_max - new_max) + jnp.sum(jnp.exp(logits - new_max[:, None]), axis=1)
        return (new_max, run_sum), None

    scan_init = (jnp.full((TOKEN_TOTAL,), -jnp.inf, jnp.float32), jnp.zeros((TOKEN_TOTAL,), jnp.float32))
    scan_out = lax.scan(max_step, scan_init, vocab_blocks)
    row_max, row_sum = scan_out[0]
    log_norm = row_max + jnp.log(row_sum)
    label_rows = jnp.take(embed_table, label_flat, axis=0)
    label_logit = jnp.sum(normed_bf.astype(jnp.float32) * label_rows.astype(jnp.float32), axis=1)
    mean_loss = jnp.sum(weight * (log_norm - label_logit))

    def grad_step(d_normed, scan_items):
        vocab_block, block_start = scan_items
        logits = jnp.dot(normed_bf, vocab_block.T, preferred_element_type=jnp.float32)
        label_hit = (label_flat[:, None] == (block_start + col_offsets)[None, :]).astype(jnp.float32)
        d_logits = (weight[:, None] * (jnp.exp(logits - log_norm[:, None]) - label_hit)).astype(jnp.bfloat16)
        d_normed = d_normed + jnp.dot(d_logits, vocab_block, preferred_element_type=jnp.float32)
        d_block = jnp.dot(d_logits.T, normed_bf, preferred_element_type=jnp.float32)
        return d_normed, d_block

    d_normed, d_blocks = lax.scan(grad_step, jnp.zeros((TOKEN_TOTAL, MODEL_DIM), jnp.float32), (vocab_blocks, block_starts))
    d_lookup = jax.ops.segment_sum(d_emb.reshape(-1, MODEL_DIM).astype(jnp.float32), tok_flat, num_segments=VOCAB_SIZE)
    d_table = d_blocks.reshape(VOCAB_SIZE, MODEL_DIM) + d_lookup
    d_hidden, d_gain, d_bias = ln_vjp(d_normed)
    return (emb_rows, mean_loss, d_hidden.astype(jnp.bfloat16).reshape(BATCH_ROWS, SEQ_LEN, MODEL_DIM), d_table, d_gain, d_bias)
```

```python
import functools

import jax
import jax.numpy as jnp
from jax import lax
from jax.experimental import pallas as pl
from jax.experimental.pallas import tpu as pltpu
from jax.sharding import PartitionSpec as P

LN_EPSILON = 1e-5
F32 = jnp.float32
BF16 = jnp.bfloat16
VMEM_LIMIT = 60 * 1024 * 1024
CHUNKS = 4


def layer_norm(inputs, ln_gain, ln_bias):
    row_mean = jnp.mean(inputs, axis=-1, keepdims=True)
    centred = inputs - row_mean
    row_var = jnp.mean(centred * centred, axis=-1, keepdims=True)
    return centred * lax.rsqrt(row_var + LN_EPSILON) * ln_gain + ln_bias


def logits_body(*refs, sub, n_sub):
    e_ref, z_ref = refs[:2]
    lt_ref, zo_ref, m_ref, s_ref = refs[-4:]
    z = z_ref[...]
    zo_ref[...] = z
    m = s = None
    for j in range(n_sub):
        rows = slice(j * sub, (j + 1) * sub)
        l = lax.dot_general(e_ref[rows, :], z, (((1,), (1,)), ((), ())), preferred_element_type=F32)
        lt_ref[rows, :] = l
        m_here = jnp.max(l, axis=0, keepdims=True)
        if m is None:
            m_new = m_here
            s = jnp.sum(jnp.exp(l - m_new), axis=0, keepdims=True)
        else:
            m_new = jnp.maximum(m, m_here)
            s = s * jnp.exp(m - m_new) + jnp.sum(jnp.exp(l - m_new), axis=0, keepdims=True)
        m = m_new
    m_ref[...] = m
    s_ref[...] = s


def logits_pass(e, z, carry, chunk, total, pt=512, sub=256):
    n_v, dim = e.shape
    n_p = z.shape[0]
    steps = n_p // pt
    first = chunk * steps
    in_specs = [pl.BlockSpec((n_v, dim), lambda i: (0, 0), pipeline_mode=pl.Buffered(1)), pl.BlockSpec((pt, dim), lambda i: (i, 0))]
    operands = [e, z]
    aliases = {}
    if carry is not None:
        in_specs += [pl.BlockSpec(memory_space=pl.ANY)] * 2
        operands += list(carry)
        aliases = {2: 0, 3: 1}
    return pl.pallas_call(
        functools.partial(logits_body, sub=sub, n_sub=n_v // sub),
        grid=(steps,),
        in_specs=in_specs,
        out_specs=[
            pl.BlockSpec((n_v, pt), lambda i: (0, i + first)),
            pl.BlockSpec((pt, dim), lambda i: (i + first, 0)),
            pl.BlockSpec((1, pt), lambda i: (0, i)),
            pl.BlockSpec((1, pt), lambda i: (0, i)),
        ],
        out_shape=[
            jax.ShapeDtypeStruct((n_v, total), F32),
            jax.ShapeDtypeStruct((total, dim), BF16),
            jax.ShapeDtypeStruct((1, n_p), F32),
            jax.ShapeDtypeStruct((1, n_p), F32),
        ],
        input_output_aliases=aliases,
        compiler_params=pltpu.CompilerParams(vmem_limit_bytes=VMEM_LIMIT, dimension_semantics=("arbitrary",)),
        cost_estimate=pl.CostEstimate(flops=2 * n_v * n_p * dim, bytes_accessed=4 * n_v * n_p + 2 * n_v * dim, transcendentals=n_v * n_p),
        name="logits_pass",
    )(*operands)


def table_grad_body(base_ref, lt_ref, z_ref, lse_ref, w_ref, y_ref, acc_ref, ll_ref, *, sub, n_sub):
    @pl.when(pl.program_id(0) == 0)
    def _():
        acc_ref[...] = jnp.zeros_like(acc_ref)

    lse = lse_ref[...]
    w = w_ref[...]
    y = y_ref[...] - base_ref[0]
    z = z_ref[...]
    row_ids = lax.broadcasted_iota(jnp.int32, (sub, z.shape[0]), 0)
    label_logit = jnp.zeros_like(lse)
    for j in range(n_sub):
        rows = slice(j * sub, (j + 1) * sub)
        l = lt_ref[rows, :]
        p = jnp.exp(l - lse)
        hit = row_ids == (y - j * sub)
        d = (w * jnp.where(hit, p - 1.0, p)).astype(BF16)
        label_logit = label_logit + jnp.sum(jnp.where(hit, l, 0.0), axis=0, keepdims=True)
        acc_ref[rows, :] += jnp.dot(d, z, preferred_element_type=F32)
    ll_ref[...] = label_logit


def table_grad(base, lt, z, lse, w, y, pt=1024, sub=256):
    n_v, n_p = lt.shape
    dim = z.shape[1]
    row = pl.BlockSpec((1, pt), lambda i, b: (0, i))
    return pl.pallas_call(
        functools.partial(table_grad_body, sub=sub, n_sub=n_v // sub),
        grid_spec=pltpu.PrefetchScalarGridSpec(
            num_scalar_prefetch=1,
            grid=(n_p // pt,),
            in_specs=[pl.BlockSpec((n_v, pt), lambda i, b: (0, i)), pl.BlockSpec((pt, dim), lambda i, b: (i, 0)), row, row, row],
            out_specs=[pl.BlockSpec((n_v, dim), lambda i, b: (0, 0), pipeline_mode=pl.Buffered(1)), row],
        ),
        out_shape=[jax.ShapeDtypeStruct((n_v, dim), F32), jax.ShapeDtypeStruct((1, n_p), F32)],
        compiler_params=pltpu.CompilerParams(vmem_limit_bytes=VMEM_LIMIT, dimension_semantics=("arbitrary",)),
        cost_estimate=pl.CostEstimate(flops=2 * n_v * n_p * dim, bytes_accessed=4 * n_v * n_p, transcendentals=n_v * n_p),
        name="table_grad",
    )(base, lt, z, lse, w, y)


def hidden_grad_body(base_ref, z_ref, e_ref, lse_ref, w_ref, y_ref, acc_ref, *, tp, n_tp, tv):
    i = pl.program_id(0)

    @pl.when(i == 0)
    def _():
        acc_ref[...] = jnp.zeros_like(acc_ref)

    e = e_ref[...]
    base = base_ref[0] + i * tv
    col_ids = lax.broadcasted_iota(jnp.int32, (tp, tv), 1)
    for j in range(n_tp):
        rows = slice(j * tp, (j + 1) * tp)
        l = lax.dot_general(z_ref[rows, :], e, (((1,), (1,)), ((), ())), preferred_element_type=F32)
        p = jnp.exp(l - lse_ref[rows, :])
        hit = col_ids == (y_ref[rows, :] - base)
        d = (w_ref[rows, :] * jnp.where(hit, p - 1.0, p)).astype(BF16)
        acc_ref[rows, :e.shape[1]] += jnp.dot(d, e, preferred_element_type=F32)


def hidden_grad(base, z, e, lse, w, y, tp=512, tv=768):
    n_v, dim = e.shape
    n_p = z.shape[0]
    wide = pl.cdiv(dim, 128) * 128
    col = pl.BlockSpec((n_p, 1), lambda i, b: (0, 0))
    return pl.pallas_call(
        functools.partial(hidden_grad_body, tp=tp, n_tp=n_p // tp, tv=tv),
        grid_spec=pltpu.PrefetchScalarGridSpec(
            num_scalar_prefetch=1,
            grid=(n_v // tv,),
            in_specs=[pl.BlockSpec((n_p, dim), lambda i, b: (0, 0)), pl.BlockSpec((tv, dim), lambda i, b: (i, 0)), col, col, col],
            out_specs=pl.BlockSpec((n_p, wide), lambda i, b: (0, 0), pipeline_mode=pl.Buffered(1)),
        ),
        out_shape=jax.ShapeDtypeStruct((n_p, wide), F32),
        compiler_params=pltpu.CompilerParams(vmem_limit_bytes=VMEM_LIMIT, dimension_semantics=("arbitrary",)),
        cost_estimate=pl.CostEstimate(flops=4 * n_v * n_p * dim, bytes_accessed=2 * n_v * dim, transcendentals=n_v * n_p),
        name="hidden_grad",
    )(base, z, e, lse, w, y)


def add_rows_body(count_ref, code_ref, de_ref, grad_ref, acc_ref, rows_ref):
    b = pl.program_id(0)

    @pl.when(b == 0)
    def _():
        acc_ref[...] = grad_ref[...]

    rows_ref[...] = de_ref[...].astype(F32)

    def step(k, carry):
        code = code_ref[0, 0, k]
        src = lax.shift_right_logical(code, 12)
        dst = lax.bitwise_and(code, 4095)
        acc_ref[pl.ds(dst, 1), :] += rows_ref[pl.ds(src, 1), :]
        return carry

    lax.fori_loop(0, count_ref[b], step, 0)


def add_rows(counts, codes, d_emb, grad):
    n_b, n_p = codes.shape
    n_v, dim = grad.shape
    whole = lambda b, c: (0, 0)
    return pl.pallas_call(
        add_rows_body,
        grid_spec=pltpu.PrefetchScalarGridSpec(
            num_scalar_prefetch=1,
            grid=(n_b,),
            in_specs=[
                pl.BlockSpec((1, 1, n_p), lambda b, c: (b, 0, 0), memory_space=pltpu.SMEM),
                pl.BlockSpec((n_p, dim), lambda b, c: (b, 0)),
                pl.BlockSpec((n_v, dim), whole, pipeline_mode=pl.Buffered(1)),
            ],
            out_specs=pl.BlockSpec((n_v, dim), whole, pipeline_mode=pl.Buffered(1)),
            scratch_shapes=[pltpu.VMEM((n_p, dim), F32)],
        ),
        out_shape=jax.ShapeDtypeStruct((n_v, dim), F32),
        compiler_params=pltpu.CompilerParams(vmem_limit_bytes=VMEM_LIMIT, dimension_semantics=("arbitrary",)),
        cost_estimate=pl.CostEstimate(flops=10**10, bytes_accessed=2 * n_b * n_p * dim, transcendentals=0),
        name="add_rows",
    )(counts, codes.reshape(n_b, 1, n_p), d_emb, grad)


def exchange_body(x_ref, out_ref, send_sem, recv_sem, *, axis, n_dev, split):
    me = lax.axis_index(axis)
    barrier = pltpu.get_barrier_semaphore()
    for k in range(1, n_dev):
        pl.semaphore_signal(barrier, inc=1, device_id=(lax.rem(me + k, n_dev),), device_id_type=pl.DeviceIdType.MESH)
    pl.semaphore_wait(barrier, n_dev - 1)
    copies = []
    for k in range(1, n_dev):
        to = lax.rem(me + k, n_dev)
        copy = pltpu.make_async_remote_copy(
            src_ref=x_ref.at[to] if split else x_ref.at[0],
            dst_ref=out_ref.at[me],
            send_sem=send_sem.at[k - 1],
            recv_sem=recv_sem.at[k - 1],
            device_id=(to,),
            device_id_type=pl.DeviceIdType.MESH,
        )
        copy.start()
        copies.append(copy)
    out_ref[pl.ds(me, 1)] = x_ref[pl.ds(me, 1)] if split else x_ref[...]
    for copy in copies:
        copy.wait()


def exchange(x, n_dev, split, collective_id, axis='fsdp'):
    block = x.shape[1:]
    return pl.pallas_call(
        functools.partial(exchange_body, axis=axis, n_dev=n_dev, split=split),
        in_specs=[pl.BlockSpec(memory_space=pltpu.VMEM)],
        out_specs=pl.BlockSpec(memory_space=pltpu.VMEM),
        out_shape=jax.ShapeDtypeStruct((n_dev,) + block, x.dtype),
        scratch_shapes=[pltpu.SemaphoreType.DMA((n_dev - 1,)), pltpu.SemaphoreType.DMA((n_dev - 1,))],
        compiler_params=pltpu.CompilerParams(collective_id=collective_id, has_side_effects=True),
        cost_estimate=pl.CostEstimate(flops=4 * 10**9, bytes_accessed=0, transcendentals=0),
        name="exchange",
    )(x)


def solution(mesh):
    batch_spec = P('fsdp', None)
    act_spec = P('fsdp', None, None)
    vec_spec = P('fsdp')
    n_dev = mesh.shape['fsdp']
    half = n_dev // 2
    planes = [list(range(half)), list(range(half, n_dev))]
    partner = [(i, (i + half) % n_dev) for i in range(n_dev)]

    def device_step(tokens, labels, loss_mask, hidden, d_emb, table_shard, gain_shard, bias_shard):
        _, seq, dim = hidden.shape
        n_v = table_shard.shape[0]
        feat = gain_shard.shape[0]
        total = n_dev * seq
        part = seq // CHUNKS
        me = lax.axis_index('fsdp')
        other = lax.rem(me + half, n_dev)
        plane = me // half

        small = jnp.concatenate([tokens.reshape(-1).astype(F32), labels.reshape(-1).astype(F32), loss_mask.reshape(-1).astype(F32), gain_shard, bias_shard])
        small = jnp.pad(small, (0, 4 * 1024 - small.shape[0])).reshape(1, 32, 128)
        small = exchange(small, n_dev, False, 1).reshape(n_dev, 4 * 1024)
        tok_all = small[:, :seq].astype(jnp.int32)
        label_all = small[:, seq:2 * seq].astype(jnp.int32)
        mask_all = small[:, 2 * seq:3 * seq]
        ln_gain = small[:, 3 * seq:3 * seq + feat].reshape(-1)
        ln_bias = small[:, 3 * seq + feat:3 * seq + 2 * feat].reshape(-1)
        weight_all = mask_all / jnp.sum(mask_all)

        hid = hidden.reshape(seq, dim).astype(F32)
        normed, ln_vjp = jax.vjp(layer_norm, hid, ln_gain, ln_bias)
        z = normed.astype(BF16)

        carry = None
        maxes, sums, z_parts = [], [], []
        for c in range(CHUNKS):
            z_c = lax.all_gather(z[c * part:(c + 1) * part], 'fsdp', axis=0, tiled=True)
            lt, z_all, m_c, s_c = logits_pass(table_shard, z_c, carry, c, total)
            carry = (lt, z_all)
            maxes.append(m_c)
            sums.append(s_c)
            z_parts.append(lax.dynamic_slice_in_dim(z_c, other * part, part, 0))
        z_other = jnp.concatenate(z_parts, axis=0)

        def to_owner(parts):
            return jnp.stack([p.reshape(n_dev, part) for p in parts], axis=1).reshape(n_dev, seq // 128, 128)

        pairs = jnp.concatenate([to_owner(maxes), to_owner(sums)], axis=1)
        pairs = exchange(pairs, n_dev, True, 2)
        pair_max, pair_sum = pairs[:, :seq // 128], pairs[:, seq // 128:]
        row_max = jnp.max(pair_max, axis=0)
        row_sum = jnp.sum(pair_sum * jnp.exp(pair_max - row_max[None]), axis=0)
        lse_all = exchange((row_max + jnp.log(row_sum))[None], n_dev, False, 3).reshape(n_dev, seq)

        def by_chunk(a):
            return a.reshape(n_dev, CHUNKS, part).transpose(1, 0, 2).reshape(1, total)

        base = (me * n_v).astype(jnp.int32).reshape(1)
        w_row = by_chunk(weight_all)
        d_table, label_logit = table_grad(base, lt, z_all, by_chunk(lse_all), w_row, by_chunk(label_all))
        loss_lse = jnp.sum(weight_all * lse_all)
        loss_hit = jnp.sum(w_row * label_logit)

        e_half = lax.all_gather(table_shard, 'fsdp', axis=0, tiled=True, axis_index_groups=planes)
        half_base = (plane * half * n_v).astype(jnp.int32)

        def row_of(a, d):
            return lax.dynamic_index_in_dim(a, d, 0, keepdims=False)

        def half_grad(d, z_d):
            return hidden_grad(half_base.reshape(1), z_d, e_half, row_of(lse_all, d)[:, None], row_of(weight_all, d)[:, None], row_of(label_all, d)[:, None])

        dz_other = half_grad(other, z_other)
        dz_other = lax.ppermute(dz_other, 'fsdp', partner)
        dz_own = half_grad(me, z)

        tok_own = row_of(tok_all, me)
        in_half = (tok_own // (half * n_v)) == plane
        look = jnp.concatenate([row_of(tok_all, other), tok_own]) - half_base
        found = jnp.take(e_half, jnp.clip(look, 0, half * n_v - 1), axis=0, mode='clip')
        found_other = lax.ppermute(found[:seq], 'fsdp', partner)
        emb_rows = jnp.where(in_half[:, None], found[seq:], found_other).reshape(1, seq, dim)

        de_all = lax.all_gather(d_emb.reshape(seq, dim), 'fsdp', axis=0, tiled=True)
        rel = tok_all - me * n_v
        mine = (rel >= 0) & (rel < n_v)
        upto = (jnp.arange(seq)[:, None] <= jnp.arange(seq)[None, :]).astype(BF16)
        rank = jnp.dot(mine.astype(BF16), upto, preferred_element_type=F32).astype(jnp.int32) - 1
        code = jnp.where(mine, jnp.arange(seq, dtype=jnp.int32)[None, :] * 4096 + rel, 0)
        slot = jnp.where(mine, rank, -1)
        codes = jnp.sum(jnp.where(slot[:, :, None] == jnp.arange(seq, dtype=jnp.int32)[None, None, :], code[:, :, None], 0), axis=1)
        counts = jnp.sum(mine.astype(jnp.int32), axis=1)
        d_table, dz_own = lax.optimization_barrier((d_table, dz_own))
        d_table = add_rows(counts, codes, de_all, d_table)

        d_hidden, d_gain, d_bias = ln_vjp((dz_own + dz_other)[:, :dim])
        tail = jnp.concatenate([d_gain.reshape(n_dev, feat), d_bias.reshape(n_dev, feat), jnp.broadcast_to(loss_hit, (n_dev, 8))], axis=1)
        tail = jnp.sum(exchange(tail[:, None, :], n_dev, True, 4), axis=0)[0]
        mean_loss = loss_lse - tail[2 * feat]
        return (emb_rows, mean_loss, d_hidden.astype(BF16).reshape(1, seq, dim), d_table, tail[:feat], tail[feat:2 * feat])

    return jax.shard_map(device_step, mesh=mesh, in_specs=(batch_spec, batch_spec, batch_spec, act_spec, act_spec, batch_spec, vec_spec, vec_spec), out_specs=(act_spec, P(), act_spec, batch_spec, vec_spec, vec_spec), check_vma=False)
```

```python
import functools

import jax
import jax.numpy as jnp
from jax import lax
from jax.experimental import pallas as pl
from jax.experimental.pallas import tpu as pltpu
from jax.sharding import PartitionSpec as P

LN_EPSILON = 1e-5
F32 = jnp.float32
BF16 = jnp.bfloat16
VMEM_LIMIT = 60 * 1024 * 1024
CHUNKS = 2


def layer_norm(inputs, ln_gain, ln_bias):
    row_mean = jnp.mean(inputs, axis=-1, keepdims=True)
    centred = inputs - row_mean
    row_var = jnp.mean(centred * centred, axis=-1, keepdims=True)
    return centred * lax.rsqrt(row_var + LN_EPSILON) * ln_gain + ln_bias


def logits_body(*refs, sub, n_sub):
    e_ref, z_ref = refs[:2]
    lt_ref, zo_ref, m_ref, s_ref = refs[-4:]
    z = z_ref[...]
    zo_ref[...] = z
    m = s = None
    for j in range(n_sub):
        rows = slice(j * sub, (j + 1) * sub)
        l = lax.dot_general(e_ref[rows, :], z, (((1,), (1,)), ((), ())), preferred_element_type=F32)
        lt_ref[rows, :] = l
        m_here = jnp.max(l, axis=0, keepdims=True)
        if m is None:
            m_new = m_here
            s = jnp.sum(jnp.exp(l - m_new), axis=0, keepdims=True)
        else:
            m_new = jnp.maximum(m, m_here)
            s = s * jnp.exp(m - m_new) + jnp.sum(jnp.exp(l - m_new), axis=0, keepdims=True)
        m = m_new
    m_ref[...] = m
    s_ref[...] = s


def logits_pass(e, z, carry, chunk, total, pt=1024, sub=256):
    n_v, dim = e.shape
    n_p = z.shape[0]
    steps = n_p // pt
    first = chunk * steps
    in_specs = [pl.BlockSpec((n_v, dim), lambda i: (0, 0), pipeline_mode=pl.Buffered(1)), pl.BlockSpec((pt, dim), lambda i: (i, 0))]
    operands = [e, z]
    aliases = {}
    if carry is not None:
        in_specs += [pl.BlockSpec(memory_space=pl.ANY)] * 2
        operands += list(carry)
        aliases = {2: 0, 3: 1}
    return pl.pallas_call(
        functools.partial(logits_body, sub=sub, n_sub=n_v // sub),
        grid=(steps,),
        in_specs=in_specs,
        out_specs=[
            pl.BlockSpec((n_v, pt), lambda i: (0, i + first)),
            pl.BlockSpec((pt, dim), lambda i: (i + first, 0)),
            pl.BlockSpec((1, pt), lambda i: (0, i)),
            pl.BlockSpec((1, pt), lambda i: (0, i)),
        ],
        out_shape=[
            jax.ShapeDtypeStruct((n_v, total), F32),
            jax.ShapeDtypeStruct((total, dim), BF16),
            jax.ShapeDtypeStruct((1, n_p), F32),
            jax.ShapeDtypeStruct((1, n_p), F32),
        ],
        input_output_aliases=aliases,
        compiler_params=pltpu.CompilerParams(vmem_limit_bytes=VMEM_LIMIT, dimension_semantics=("arbitrary",)),
        cost_estimate=pl.CostEstimate(flops=2 * n_v * n_p * dim, bytes_accessed=4 * n_v * n_p + 2 * n_v * dim, transcendentals=n_v * n_p),
        name="logits_pass",
    )(*operands)


def table_grad_body(base_ref, lt_ref, z_ref, lse_ref, w_ref, y_ref, acc_ref, ll_ref, *, sub, n_sub):
    @pl.when(pl.program_id(0) == 0)
    def _():
        acc_ref[...] = jnp.zeros_like(acc_ref)

    lse = lse_ref[...]
    w = w_ref[...]
    y = y_ref[...] - base_ref[0]
    z = z_ref[...]
    row_ids = lax.broadcasted_iota(jnp.int32, (sub, z.shape[0]), 0)
    label_logit = jnp.zeros_like(lse)
    for j in range(n_sub):
        rows = slice(j * sub, (j + 1) * sub)
        l = lt_ref[rows, :]
        p = jnp.exp(l - lse)
        hit = row_ids == (y - j * sub)
        d = (w * jnp.where(hit, p - 1.0, p)).astype(BF16)
        label_logit = label_logit + jnp.sum(jnp.where(hit, l, 0.0), axis=0, keepdims=True)
        acc_ref[rows, :] += jnp.dot(d, z, preferred_element_type=F32)
    ll_ref[...] = label_logit


def table_grad(base, lt, z, lse, w, y, pt=1024, sub=256):
    n_v, n_p = lt.shape
    dim = z.shape[1]
    row = pl.BlockSpec((1, pt), lambda i, b: (0, i))
    return pl.pallas_call(
        functools.partial(table_grad_body, sub=sub, n_sub=n_v // sub),
        grid_spec=pltpu.PrefetchScalarGridSpec(
            num_scalar_prefetch=1,
            grid=(n_p // pt,),
            in_specs=[pl.BlockSpec((n_v, pt), lambda i, b: (0, i)), pl.BlockSpec((pt, dim), lambda i, b: (i, 0)), row, row, row],
            out_specs=[pl.BlockSpec((n_v, dim), lambda i, b: (0, 0), pipeline_mode=pl.Buffered(1)), row],
        ),
        out_shape=[jax.ShapeDtypeStruct((n_v, dim), F32), jax.ShapeDtypeStruct((1, n_p), F32)],
        compiler_params=pltpu.CompilerParams(vmem_limit_bytes=VMEM_LIMIT, dimension_semantics=("arbitrary",)),
        cost_estimate=pl.CostEstimate(flops=2 * n_v * n_p * dim, bytes_accessed=4 * n_v * n_p, transcendentals=n_v * n_p),
        name="table_grad",
    )(base, lt, z, lse, w, y)


def hidden_grad_body(base_ref, z_ref, e_ref, lse_ref, w_ref, y_ref, acc_ref, *, tp, n_tp, tv):
    i = pl.program_id(0)

    @pl.when(i == 0)
    def _():
        acc_ref[...] = jnp.zeros_like(acc_ref)

    e = e_ref[...]
    base = base_ref[0] + i * tv
    col_ids = lax.broadcasted_iota(jnp.int32, (tp, tv), 1)
    for j in range(n_tp):
        rows = slice(j * tp, (j + 1) * tp)
        l = lax.dot_general(z_ref[rows, :], e, (((1,), (1,)), ((), ())), preferred_element_type=F32)
        p = jnp.exp(l - lse_ref[rows, :])
        hit = col_ids == (y_ref[rows, :] - base)
        d = (w_ref[rows, :] * jnp.where(hit, p - 1.0, p)).astype(BF16)
        acc_ref[rows, :e.shape[1]] += jnp.dot(d, e, preferred_element_type=F32)


def hidden_grad(base, z, e, lse, w, y, tp=512, tv=768):
    n_v, dim = e.shape
    n_p = z.shape[0]
    wide = pl.cdiv(dim, 128) * 128
    col = pl.BlockSpec((n_p, 1), lambda i, b: (0, 0))
    return pl.pallas_call(
        functools.partial(hidden_grad_body, tp=tp, n_tp=n_p // tp, tv=tv),
        grid_spec=pltpu.PrefetchScalarGridSpec(
            num_scalar_prefetch=1,
            grid=(n_v // tv,),
            in_specs=[pl.BlockSpec((n_p, dim), lambda i, b: (0, 0)), pl.BlockSpec((tv, dim), lambda i, b: (i, 0)), col, col, col],
            out_specs=pl.BlockSpec((n_p, wide), lambda i, b: (0, 0), pipeline_mode=pl.Buffered(1)),
        ),
        out_shape=jax.ShapeDtypeStruct((n_p, wide), F32),
        compiler_params=pltpu.CompilerParams(vmem_limit_bytes=VMEM_LIMIT, dimension_semantics=("arbitrary",)),
        cost_estimate=pl.CostEstimate(flops=4 * n_v * n_p * dim, bytes_accessed=2 * n_v * dim, transcendentals=n_v * n_p),
        name="hidden_grad",
    )(base, z, e, lse, w, y)


def add_rows_body(count_ref, code_ref, de_ref, grad_ref, acc_ref, rows_ref):
    b = pl.program_id(0)

    @pl.when(b == 0)
    def _():
        acc_ref[...] = grad_ref[...]

    rows_ref[...] = de_ref[...].astype(F32)

    def step(k, carry):
        code = code_ref[0, 0, k]
        src = lax.shift_right_logical(code, 12)
        dst = lax.bitwise_and(code, 4095)
        acc_ref[pl.ds(dst, 1), :] += rows_ref[pl.ds(src, 1), :]
        return carry

    lax.fori_loop(0, count_ref[b], step, 0)


def add_rows(counts, codes, d_emb, grad):
    n_b, n_p = codes.shape
    n_v, dim = grad.shape
    whole = lambda b, c: (0, 0)
    return pl.pallas_call(
        add_rows_body,
        grid_spec=pltpu.PrefetchScalarGridSpec(
            num_scalar_prefetch=1,
            grid=(n_b,),
            in_specs=[
                pl.BlockSpec((1, 1, n_p), lambda b, c: (b, 0, 0), memory_space=pltpu.SMEM),
                pl.BlockSpec((n_p, dim), lambda b, c: (b, 0)),
                pl.BlockSpec((n_v, dim), whole, pipeline_mode=pl.Buffered(1)),
            ],
            out_specs=pl.BlockSpec((n_v, dim), whole, pipeline_mode=pl.Buffered(1)),
            scratch_shapes=[pltpu.VMEM((n_p, dim), F32)],
        ),
        out_shape=jax.ShapeDtypeStruct((n_v, dim), F32),
        compiler_params=pltpu.CompilerParams(vmem_limit_bytes=VMEM_LIMIT, dimension_semantics=("arbitrary",)),
        cost_estimate=pl.CostEstimate(flops=10**10, bytes_accessed=2 * n_b * n_p * dim, transcendentals=0),
        name="add_rows",
    )(counts, codes.reshape(n_b, 1, n_p), d_emb, grad)


def place_rows_body(count_ref, code_ref, e_ref, out_ref, wide_ref, rows_ref):
    b = pl.program_id(0)

    @pl.when(b == 0)
    def _():
        wide_ref[...] = e_ref[...].astype(F32)

    rows_ref[...] = jnp.zeros_like(rows_ref)

    def step(k, carry):
        code = code_ref[0, 0, k]
        dst = lax.shift_right_logical(code, 12)
        src = lax.bitwise_and(code, 4095)
        rows_ref[pl.ds(dst, 1), :] = wide_ref[pl.ds(src, 1), :]
        return carry

    lax.fori_loop(0, count_ref[b], step, 0)
    out_ref[...] = rows_ref[...].astype(BF16)


def place_rows(counts, codes, e):
    n_b, n_p = codes.shape
    n_v, dim = e.shape
    return pl.pallas_call(
        place_rows_body,
        grid_spec=pltpu.PrefetchScalarGridSpec(
            num_scalar_prefetch=1,
            grid=(n_b,),
            in_specs=[
                pl.BlockSpec((1, 1, n_p), lambda b, c: (b, 0, 0), memory_space=pltpu.SMEM),
                pl.BlockSpec((n_v, dim), lambda b, c: (0, 0), pipeline_mode=pl.Buffered(1)),
            ],
            out_specs=pl.BlockSpec((n_p, dim), lambda b, c: (b, 0)),
            scratch_shapes=[pltpu.VMEM((n_v, dim), F32), pltpu.VMEM((n_p, dim), F32)],
        ),
        out_shape=jax.ShapeDtypeStruct((n_b * n_p, dim), BF16),
        compiler_params=pltpu.CompilerParams(vmem_limit_bytes=VMEM_LIMIT, dimension_semantics=("arbitrary",)),
        cost_estimate=pl.CostEstimate(flops=10**10, bytes_accessed=2 * n_b * n_p * dim, transcendentals=0),
        name="place_rows",
    )(counts, codes.reshape(n_b, 1, n_p), e)


def exchange_body(x_ref, out_ref, send_sem, recv_sem, *, axis, n_dev, split):
    me = lax.axis_index(axis)
    barrier = pltpu.get_barrier_semaphore()
    for k in range(1, n_dev):
        pl.semaphore_signal(barrier, inc=1, device_id=(lax.rem(me + k, n_dev),), device_id_type=pl.DeviceIdType.MESH)
    pl.semaphore_wait(barrier, n_dev - 1)
    copies = []
    for k in range(1, n_dev):
        to = lax.rem(me + k, n_dev)
        copy = pltpu.make_async_remote_copy(
            src_ref=x_ref.at[to] if split else x_ref.at[0],
            dst_ref=out_ref.at[me],
            send_sem=send_sem.at[k - 1],
            recv_sem=recv_sem.at[k - 1],
            device_id=(to,),
            device_id_type=pl.DeviceIdType.MESH,
        )
        copy.start()
        copies.append(copy)
    out_ref[pl.ds(me, 1)] = x_ref[pl.ds(me, 1)] if split else x_ref[...]
    for copy in copies:
        copy.wait()


def exchange(x, n_dev, split, collective_id, axis='fsdp'):
    block = x.shape[1:]
    return pl.pallas_call(
        functools.partial(exchange_body, axis=axis, n_dev=n_dev, split=split),
        in_specs=[pl.BlockSpec(memory_space=pltpu.VMEM)],
        out_specs=pl.BlockSpec(memory_space=pltpu.VMEM),
        out_shape=jax.ShapeDtypeStruct((n_dev,) + block, x.dtype),
        scratch_shapes=[pltpu.SemaphoreType.DMA((n_dev - 1,)), pltpu.SemaphoreType.DMA((n_dev - 1,))],
        compiler_params=pltpu.CompilerParams(collective_id=collective_id, has_side_effects=True),
        cost_estimate=pl.CostEstimate(flops=4 * 10**9, bytes_accessed=0, transcendentals=0),
        name="exchange",
    )(x)


def solution(mesh):
    batch_spec = P('fsdp', None)
    act_spec = P('fsdp', None, None)
    vec_spec = P('fsdp')
    n_dev = mesh.shape['fsdp']
    half = n_dev // 2
    planes = [list(range(half)), list(range(half, n_dev))]
    partner = [(i, (i + half) % n_dev) for i in range(n_dev)]

    def device_step(tokens, labels, loss_mask, hidden, d_emb, table_shard, gain_shard, bias_shard):
        _, seq, dim = hidden.shape
        n_v = table_shard.shape[0]
        feat = gain_shard.shape[0]
        total = n_dev * seq
        part = seq // CHUNKS
        me = lax.axis_index('fsdp')
        other = lax.rem(me + half, n_dev)
        plane = me // half

        small = jnp.concatenate([tokens.reshape(-1).astype(F32), labels.reshape(-1).astype(F32), loss_mask.reshape(-1).astype(F32), gain_shard, bias_shard])
        small = jnp.pad(small, (0, 4 * 1024 - small.shape[0])).reshape(1, 32, 128)
        small = exchange(small, n_dev, False, 1).reshape(n_dev, 4 * 1024)
        tok_all = small[:, :seq].astype(jnp.int32)
        label_all = small[:, seq:2 * seq].astype(jnp.int32)
        mask_all = small[:, 2 * seq:3 * seq]
        ln_gain = small[:, 3 * seq:3 * seq + feat].reshape(-1)
        ln_bias = small[:, 3 * seq + feat:3 * seq + 2 * feat].reshape(-1)
        weight_all = mask_all / jnp.sum(mask_all)

        hid = hidden.reshape(seq, dim).astype(F32)
        normed, ln_vjp = jax.vjp(layer_norm, hid, ln_gain, ln_bias)
        z = normed.astype(BF16)

        rel = tok_all - me * n_v
        mine = (rel >= 0) & (rel < n_v)
        upto = (jnp.arange(seq)[:, None] <= jnp.arange(seq)[None, :]).astype(BF16)
        rank = jnp.dot(mine.astype(BF16), upto, preferred_element_type=F32).astype(jnp.int32) - 1
        code = jnp.where(mine, jnp.arange(seq, dtype=jnp.int32)[None, :] * 4096 + rel, 0)
        slot = jnp.where(mine, rank, -1)
        codes = jnp.sum(jnp.where(slot[:, :, None] == jnp.arange(seq, dtype=jnp.int32)[None, None, :], code[:, :, None], 0), axis=1)
        counts = jnp.sum(mine.astype(jnp.int32), axis=1)
        emb_part = place_rows(counts, codes, table_shard)

        carry = None
        maxes, sums, z_parts = [], [], []
        for c in range(CHUNKS):
            z_c = lax.all_gather(z[c * part:(c + 1) * part], 'fsdp', axis=0, tiled=True)
            lt, z_all, m_c, s_c = logits_pass(table_shard, z_c, carry, c, total)
            carry = (lt, z_all)
            maxes.append(m_c)
            sums.append(s_c)
            z_parts.append(lax.dynamic_slice_in_dim(z_c, other * part, part, 0))
        z_other = jnp.concatenate(z_parts, axis=0)

        def to_owner(parts):
            return jnp.stack([p.reshape(n_dev, part) for p in parts], axis=1).reshape(n_dev, seq // 128, 128)

        pairs = jnp.concatenate([to_owner(maxes), to_owner(sums)], axis=1)
        pairs = exchange(pairs, n_dev, True, 2)
        pair_max, pair_sum = pairs[:, :seq // 128], pairs[:, seq // 128:]
        row_max = jnp.max(pair_max, axis=0)
        row_sum = jnp.sum(pair_sum * jnp.exp(pair_max - row_max[None]), axis=0)
        lse_all = exchange((row_max + jnp.log(row_sum))[None], n_dev, False, 3).reshape(n_dev, seq)

        def by_chunk(a):
            return a.reshape(n_dev, CHUNKS, part).transpose(1, 0, 2).reshape(1, total)

        base = (me * n_v).astype(jnp.int32).reshape(1)
        w_row = by_chunk(weight_all)
        d_table, label_logit = table_grad(base, lt, z_all, by_chunk(lse_all), w_row, by_chunk(label_all))
        loss_lse = jnp.sum(weight_all * lse_all)
        loss_hit = jnp.sum(w_row * label_logit)

        e_half = lax.all_gather(table_shard, 'fsdp', axis=0, tiled=True, axis_index_groups=planes)
        half_base = (plane * half * n_v).astype(jnp.int32)

        def row_of(a, d):
            return lax.dynamic_index_in_dim(a, d, 0, keepdims=False)

        def half_grad(d, z_d):
            return hidden_grad(half_base.reshape(1), z_d, e_half, row_of(lse_all, d)[:, None], row_of(weight_all, d)[:, None], row_of(label_all, d)[:, None])

        z_other, d_table = lax.optimization_barrier((z_other, d_table))
        dz_other = half_grad(other, z_other)
        emb_part, dz_other = lax.optimization_barrier((emb_part, dz_other))
        emb_rows = lax.psum_scatter(emb_part, 'fsdp', scatter_dimension=0, tiled=True).reshape(1, seq, dim)
        dz_other = lax.ppermute(dz_other, 'fsdp', partner)
        dz_own = half_grad(me, z)

        de_all = lax.all_gather(d_emb.reshape(seq, dim), 'fsdp', axis=0, tiled=True)
        d_table, dz_own = lax.optimization_barrier((d_table, dz_own))
        d_table = add_rows(counts, codes, de_all, d_table)

        d_hidden, d_gain, d_bias = ln_vjp((dz_own + dz_other)[:, :dim])
        tail = jnp.concatenate([d_gain.reshape(n_dev, feat), d_bias.reshape(n_dev, feat), jnp.broadcast_to(loss_hit, (n_dev, 8))], axis=1)
        tail = jnp.sum(exchange(tail[:, None, :], n_dev, True, 4), axis=0)[0]
        mean_loss = loss_lse - tail[2 * feat]
        return (emb_rows, mean_loss, d_hidden.astype(BF16).reshape(1, seq, dim), d_table, tail[:feat], tail[feat:2 * feat])

    return jax.shard_map(device_step, mesh=mesh, in_specs=(batch_spec, batch_spec, batch_spec, act_spec, act_spec, batch_spec, vec_spec, vec_spec), out_specs=(act_spec, P(), act_spec, batch_spec, vec_spec, vec_spec), check_vma=False)
```

```python
import functools

import jax
import jax.numpy as jnp
from jax import lax
from jax.experimental import pallas as pl
from jax.experimental.pallas import tpu as pltpu
from jax.sharding import PartitionSpec as P

LN_EPSILON = 1e-5
F32 = jnp.float32
BF16 = jnp.bfloat16
VMEM_LIMIT = 60 * 1024 * 1024
CHUNKS = 2


def layer_norm(inputs, ln_gain, ln_bias):
    row_mean = jnp.mean(inputs, axis=-1, keepdims=True)
    centred = inputs - row_mean
    row_var = jnp.mean(centred * centred, axis=-1, keepdims=True)
    return centred * lax.rsqrt(row_var + LN_EPSILON) * ln_gain + ln_bias


def logits_body(*refs, sub, n_sub):
    e_ref, z_ref = refs[:2]
    lt_ref, zo_ref, m_ref, s_ref = refs[-4:]
    z = z_ref[...]
    zo_ref[...] = z
    m = s = None
    for j in range(n_sub):
        rows = slice(j * sub, (j + 1) * sub)
        l = lax.dot_general(e_ref[rows, :], z, (((1,), (1,)), ((), ())), preferred_element_type=F32)
        lt_ref[rows, :] = l
        m_here = jnp.max(l, axis=0, keepdims=True)
        if m is None:
            m_new = m_here
            s = jnp.sum(jnp.exp(l - m_new), axis=0, keepdims=True)
        else:
            m_new = jnp.maximum(m, m_here)
            s = s * jnp.exp(m - m_new) + jnp.sum(jnp.exp(l - m_new), axis=0, keepdims=True)
        m = m_new
    m_ref[...] = m
    s_ref[...] = s


def logits_pass(e, z, carry, chunk, total, pt=1024, sub=256):
    n_v, dim = e.shape
    n_p = z.shape[0]
    steps = n_p // pt
    first = chunk * steps
    in_specs = [pl.BlockSpec((n_v, dim), lambda i: (0, 0), pipeline_mode=pl.Buffered(1)), pl.BlockSpec((pt, dim), lambda i: (i, 0))]
    operands = [e, z]
    aliases = {}
    if carry is not None:
        in_specs += [pl.BlockSpec(memory_space=pl.ANY)] * 2
        operands += list(carry)
        aliases = {2: 0, 3: 1}
    return pl.pallas_call(
        functools.partial(logits_body, sub=sub, n_sub=n_v // sub),
        grid=(steps,),
        in_specs=in_specs,
        out_specs=[
            pl.BlockSpec((n_v, pt), lambda i: (0, i + first)),
            pl.BlockSpec((pt, dim), lambda i: (i + first, 0)),
            pl.BlockSpec((1, pt), lambda i: (0, i)),
            pl.BlockSpec((1, pt), lambda i: (0, i)),
        ],
        out_shape=[
            jax.ShapeDtypeStruct((n_v, total), F32),
            jax.ShapeDtypeStruct((total, dim), BF16),
            jax.ShapeDtypeStruct((1, n_p), F32),
            jax.ShapeDtypeStruct((1, n_p), F32),
        ],
        input_output_aliases=aliases,
        compiler_params=pltpu.CompilerParams(vmem_limit_bytes=VMEM_LIMIT, dimension_semantics=("arbitrary",)),
        cost_estimate=pl.CostEstimate(flops=2 * n_v * n_p * dim, bytes_accessed=4 * n_v * n_p + 2 * n_v * dim, transcendentals=n_v * n_p),
        name="logits_pass",
    )(*operands)


def table_grad_body(base_ref, lt_ref, z_ref, lse_ref, w_ref, y_ref, acc_ref, ll_ref, *, sub, n_sub):
    @pl.when(pl.program_id(0) == 0)
    def _():
        acc_ref[...] = jnp.zeros_like(acc_ref)

    lse = lse_ref[...]
    w = w_ref[...]
    y = y_ref[...] - base_ref[0]
    z = z_ref[...]
    row_ids = lax.broadcasted_iota(jnp.int32, (sub, z.shape[0]), 0)
    label_logit = jnp.zeros_like(lse)
    for j in range(n_sub):
        rows = slice(j * sub, (j + 1) * sub)
        l = lt_ref[rows, :]
        p = jnp.exp(l - lse)
        hit = row_ids == (y - j * sub)
        d = (w * jnp.where(hit, p - 1.0, p)).astype(BF16)
        label_logit = label_logit + jnp.sum(jnp.where(hit, l, 0.0), axis=0, keepdims=True)
        acc_ref[rows, :] += jnp.dot(d, z, preferred_element_type=F32)
    ll_ref[...] = label_logit


def table_grad(base, lt, z, lse, w, y, pt=1024, sub=256):
    n_v, n_p = lt.shape
    dim = z.shape[1]
    row = pl.BlockSpec((1, pt), lambda i, b: (0, i))
    return pl.pallas_call(
        functools.partial(table_grad_body, sub=sub, n_sub=n_v // sub),
        grid_spec=pltpu.PrefetchScalarGridSpec(
            num_scalar_prefetch=1,
            grid=(n_p // pt,),
            in_specs=[pl.BlockSpec((n_v, pt), lambda i, b: (0, i)), pl.BlockSpec((pt, dim), lambda i, b: (i, 0)), row, row, row],
            out_specs=[pl.BlockSpec((n_v, dim), lambda i, b: (0, 0), pipeline_mode=pl.Buffered(1)), row],
        ),
        out_shape=[jax.ShapeDtypeStruct((n_v, dim), F32), jax.ShapeDtypeStruct((1, n_p), F32)],
        compiler_params=pltpu.CompilerParams(vmem_limit_bytes=VMEM_LIMIT, dimension_semantics=("arbitrary",)),
        cost_estimate=pl.CostEstimate(flops=2 * n_v * n_p * dim, bytes_accessed=4 * n_v * n_p, transcendentals=n_v * n_p),
        name="table_grad",
    )(base, lt, z, lse, w, y)


def hidden_grad_body(base_ref, z_ref, e_ref, lse_ref, w_ref, y_ref, acc_ref, *, tp, n_tp, tv):
    i = pl.program_id(0)

    @pl.when(i == 0)
    def _():
        acc_ref[...] = jnp.zeros_like(acc_ref)

    e = e_ref[...]
    base = base_ref[0] + i * tv
    col_ids = lax.broadcasted_iota(jnp.int32, (tp, tv), 1)
    for j in range(n_tp):
        rows = slice(j * tp, (j + 1) * tp)
        l = lax.dot_general(z_ref[rows, :], e, (((1,), (1,)), ((), ())), preferred_element_type=F32)
        p = jnp.exp(l - lse_ref[rows, :])
        hit = col_ids == (y_ref[rows, :] - base)
        d = (w_ref[rows, :] * jnp.where(hit, p - 1.0, p)).astype(BF16)
        acc_ref[rows, :e.shape[1]] += jnp.dot(d, e, preferred_element_type=F32)


def hidden_grad(base, z, e, lse, w, y, tp=512, tv=768):
    n_v, dim = e.shape
    n_p = z.shape[0]
    wide = pl.cdiv(dim, 128) * 128
    col = pl.BlockSpec((n_p, 1), lambda i, b: (0, 0))
    return pl.pallas_call(
        functools.partial(hidden_grad_body, tp=tp, n_tp=n_p // tp, tv=tv),
        grid_spec=pltpu.PrefetchScalarGridSpec(
            num_scalar_prefetch=1,
            grid=(n_v // tv,),
            in_specs=[pl.BlockSpec((n_p, dim), lambda i, b: (0, 0)), pl.BlockSpec((tv, dim), lambda i, b: (i, 0)), col, col, col],
            out_specs=pl.BlockSpec((n_p, wide), lambda i, b: (0, 0), pipeline_mode=pl.Buffered(1)),
        ),
        out_shape=jax.ShapeDtypeStruct((n_p, wide), F32),
        compiler_params=pltpu.CompilerParams(vmem_limit_bytes=VMEM_LIMIT, dimension_semantics=("arbitrary",)),
        cost_estimate=pl.CostEstimate(flops=4 * n_v * n_p * dim, bytes_accessed=2 * n_v * dim, transcendentals=n_v * n_p),
        name="hidden_grad",
    )(base, z, e, lse, w, y)


def add_rows_body(count_ref, code_ref, de_ref, grad_ref, acc_ref, rows_ref):
    b = pl.program_id(0)

    @pl.when(b == 0)
    def _():
        acc_ref[...] = grad_ref[...]

    rows_ref[...] = de_ref[...].astype(F32)

    def step(k, carry):
        code = code_ref[0, 0, k]
        src = lax.shift_right_logical(code, 12)
        dst = lax.bitwise_and(code, 4095)
        acc_ref[pl.ds(dst, 1), :] += rows_ref[pl.ds(src, 1), :]
        return carry

    lax.fori_loop(0, count_ref[b], step, 0)


def add_rows(counts, codes, d_emb, grad):
    n_b, n_p = codes.shape
    n_v, dim = grad.shape
    whole = lambda b, c: (0, 0)
    return pl.pallas_call(
        add_rows_body,
        grid_spec=pltpu.PrefetchScalarGridSpec(
            num_scalar_prefetch=1,
            grid=(n_b,),
            in_specs=[
                pl.BlockSpec((1, 1, n_p), lambda b, c: (b, 0, 0), memory_space=pltpu.SMEM),
                pl.BlockSpec((n_p, dim), lambda b, c: (b, 0)),
                pl.BlockSpec((n_v, dim), whole, pipeline_mode=pl.Buffered(1)),
            ],
            out_specs=pl.BlockSpec((n_v, dim), whole, pipeline_mode=pl.Buffered(1)),
            scratch_shapes=[pltpu.VMEM((n_p, dim), F32)],
        ),
        out_shape=jax.ShapeDtypeStruct((n_v, dim), F32),
        compiler_params=pltpu.CompilerParams(vmem_limit_bytes=VMEM_LIMIT, dimension_semantics=("arbitrary",)),
        cost_estimate=pl.CostEstimate(flops=10**10, bytes_accessed=2 * n_b * n_p * dim, transcendentals=0),
        name="add_rows",
    )(counts, codes.reshape(n_b, 1, n_p), d_emb, grad)


def place_rows_body(count_ref, code_ref, e_ref, first_ref, second_ref, wide_ref, rows_ref):
    b = pl.program_id(0)
    n_b = pl.num_programs(0)
    n_p = first_ref.shape[0]

    @pl.when(b == 0)
    def _():
        rows_ref[...] = jnp.zeros_like(rows_ref)

    wide_ref[...] = e_ref[...].astype(F32)

    for part in range(2):
        def step(k, carry):
            code = code_ref[0, part, k]
            dst = lax.shift_right_logical(code, 12) + part * n_p
            src = lax.bitwise_and(code, 4095)
            rows_ref[pl.ds(dst, 1), :] = wide_ref[pl.ds(src, 1), :]
            return carry

        lax.fori_loop(0, count_ref[part * n_b + b], step, 0)

    @pl.when(b == n_b - 1)
    def _():
        dim = rows_ref.shape[1]
        first_ref[:, :dim] = rows_ref[:n_p, :].astype(BF16)
        second_ref[:, :dim] = rows_ref[n_p:, :].astype(BF16)


def place_rows(counts, codes, e):
    _, n_b, n_p = codes.shape
    dim = e.shape[1]
    n_v = e.shape[0] // n_b
    wide = pl.cdiv(dim, 128) * 128
    out = pl.BlockSpec((n_p, wide), lambda b, c: (0, 0), pipeline_mode=pl.Buffered(1))
    return pl.pallas_call(
        place_rows_body,
        grid_spec=pltpu.PrefetchScalarGridSpec(
            num_scalar_prefetch=1,
            grid=(n_b,),
            in_specs=[
                pl.BlockSpec((1, 2, n_p), lambda b, c: (b, 0, 0), memory_space=pltpu.SMEM),
                pl.BlockSpec((n_v, dim), lambda b, c: (b, 0)),
            ],
            out_specs=[out, out],
            scratch_shapes=[pltpu.VMEM((n_v, dim), F32), pltpu.VMEM((2 * n_p, dim), F32)],
        ),
        out_shape=[jax.ShapeDtypeStruct((n_p, wide), BF16)] * 2,
        compiler_params=pltpu.CompilerParams(vmem_limit_bytes=VMEM_LIMIT, dimension_semantics=("arbitrary",)),
        cost_estimate=pl.CostEstimate(flops=10**10, bytes_accessed=2 * n_b * n_v * dim, transcendentals=0),
        name="place_rows",
    )(counts.reshape(-1), codes.transpose(1, 0, 2), e)


def exchange_body(x_ref, out_ref, send_sem, recv_sem, *, axis, n_dev, split):
    me = lax.axis_index(axis)
    barrier = pltpu.get_barrier_semaphore()
    for k in range(1, n_dev):
        pl.semaphore_signal(barrier, inc=1, device_id=(lax.rem(me + k, n_dev),), device_id_type=pl.DeviceIdType.MESH)
    pl.semaphore_wait(barrier, n_dev - 1)
    copies = []
    for k in range(1, n_dev):
        to = lax.rem(me + k, n_dev)
        copy = pltpu.make_async_remote_copy(
            src_ref=x_ref.at[to] if split else x_ref.at[0],
            dst_ref=out_ref.at[me],
            send_sem=send_sem.at[k - 1],
            recv_sem=recv_sem.at[k - 1],
            device_id=(to,),
            device_id_type=pl.DeviceIdType.MESH,
        )
        copy.start()
        copies.append(copy)
    out_ref[pl.ds(me, 1)] = x_ref[pl.ds(me, 1)] if split else x_ref[...]
    for copy in copies:
        copy.wait()


def exchange(x, n_dev, split, collective_id, axis='fsdp'):
    block = x.shape[1:]
    return pl.pallas_call(
        functools.partial(exchange_body, axis=axis, n_dev=n_dev, split=split),
        in_specs=[pl.BlockSpec(memory_space=pltpu.VMEM)],
        out_specs=pl.BlockSpec(memory_space=pltpu.VMEM),
        out_shape=jax.ShapeDtypeStruct((n_dev,) + block, x.dtype),
        scratch_shapes=[pltpu.SemaphoreType.DMA((n_dev - 1,)), pltpu.SemaphoreType.DMA((n_dev - 1,))],
        compiler_params=pltpu.CompilerParams(collective_id=collective_id, has_side_effects=True),
        cost_estimate=pl.CostEstimate(flops=4 * 10**9, bytes_accessed=0, transcendentals=0),
        name="exchange",
    )(x)


def solution(mesh):
    batch_spec = P('fsdp', None)
    act_spec = P('fsdp', None, None)
    vec_spec = P('fsdp')
    n_dev = mesh.shape['fsdp']
    half = n_dev // 2
    planes = [list(range(half)), list(range(half, n_dev))]
    partner = [(i, (i + half) % n_dev) for i in range(n_dev)]

    def device_step(tokens, labels, loss_mask, hidden, d_emb, table_shard, gain_shard, bias_shard):
        _, seq, dim = hidden.shape
        n_v = table_shard.shape[0]
        feat = gain_shard.shape[0]
        total = n_dev * seq
        part = seq // CHUNKS
        me = lax.axis_index('fsdp')
        other = lax.rem(me + half, n_dev)
        plane = me // half

        small = jnp.concatenate([tokens.reshape(-1).astype(F32), labels.reshape(-1).astype(F32), loss_mask.reshape(-1).astype(F32), gain_shard, bias_shard])
        small = jnp.pad(small, (0, 4 * 1024 - small.shape[0])).reshape(1, 32, 128)
        small = exchange(small, n_dev, False, 1).reshape(n_dev, 4 * 1024)
        tok_all = small[:, :seq].astype(jnp.int32)
        label_all = small[:, seq:2 * seq].astype(jnp.int32)
        mask_all = small[:, 2 * seq:3 * seq]
        ln_gain = small[:, 3 * seq:3 * seq + feat].reshape(-1)
        ln_bias = small[:, 3 * seq + feat:3 * seq + 2 * feat].reshape(-1)
        weight_all = mask_all / jnp.sum(mask_all)

        hid = hidden.reshape(seq, dim).astype(F32)
        normed, ln_vjp = jax.vjp(layer_norm, hid, ln_gain, ln_bias)
        z = normed.astype(BF16)

        def row_of(a, d):
            return lax.dynamic_index_in_dim(a, d, 0, keepdims=False)

        upto = (jnp.arange(seq)[:, None] <= jnp.arange(seq)[None, :]).astype(BF16)

        def pack(rel):
            hit = (rel >= 0) & (rel < n_v)
            rank = jnp.dot(hit.astype(BF16), upto, preferred_element_type=F32).astype(jnp.int32) - 1
            code = jnp.where(hit, jnp.arange(seq, dtype=jnp.int32)[None, :] * 4096 + rel, 0)
            slot = jnp.where(hit, rank, -1)
            codes = jnp.sum(jnp.where(slot[:, :, None] == jnp.arange(seq, dtype=jnp.int32)[None, None, :], code[:, :, None], 0), axis=1)
            return codes, jnp.sum(hit.astype(jnp.int32), axis=1)

        codes, counts = pack(tok_all - me * n_v)
        tok_own = row_of(tok_all, me)
        block_start = (plane * half + jnp.arange(half, dtype=jnp.int32)) * n_v
        look = jnp.stack([row_of(tok_all, other), tok_own])[:, None, :] - block_start[None, :, None]
        look_codes, look_counts = pack(look.reshape(2 * half, seq))
        in_half = (tok_own // (half * n_v)) == plane

        carry = None
        maxes, sums, z_parts = [], [], []
        for c in range(CHUNKS):
            z_c = lax.all_gather(z[c * part:(c + 1) * part], 'fsdp', axis=0, tiled=True)
            if c == 0:
                z_c, codes, counts, look_codes, look_counts = lax.optimization_barrier((z_c, codes, counts, look_codes, look_counts))
            lt, z_all, m_c, s_c = logits_pass(table_shard, z_c, carry, c, total)
            carry = (lt, z_all)
            maxes.append(m_c)
            sums.append(s_c)
            z_parts.append(lax.dynamic_slice_in_dim(z_c, other * part, part, 0))
        z_other = jnp.concatenate(z_parts, axis=0)

        def to_owner(parts):
            return jnp.stack([p.reshape(n_dev, part) for p in parts], axis=1).reshape(n_dev, seq // 128, 128)

        pairs = jnp.concatenate([to_owner(maxes), to_owner(sums)], axis=1)
        pairs = exchange(pairs, n_dev, True, 2)
        pair_max, pair_sum = pairs[:, :seq // 128], pairs[:, seq // 128:]
        row_max = jnp.max(pair_max, axis=0)
        row_sum = jnp.sum(pair_sum * jnp.exp(pair_max - row_max[None]), axis=0)
        lse_all = exchange((row_max + jnp.log(row_sum))[None], n_dev, False, 3).reshape(n_dev, seq)

        def by_chunk(a):
            return a.reshape(n_dev, CHUNKS, part).transpose(1, 0, 2).reshape(1, total)

        base = (me * n_v).astype(jnp.int32).reshape(1)
        w_row = by_chunk(weight_all)
        d_table, label_logit = table_grad(base, lt, z_all, by_chunk(lse_all), w_row, by_chunk(label_all))
        loss_lse = jnp.sum(weight_all * lse_all)
        loss_hit = jnp.sum(w_row * label_logit)

        e_half = lax.all_gather(table_shard, 'fsdp', axis=0, tiled=True, axis_index_groups=planes)
        half_base = (plane * half * n_v).astype(jnp.int32)

        def half_grad(d, z_d):
            return hidden_grad(half_base.reshape(1), z_d, e_half, row_of(lse_all, d)[:, None], row_of(weight_all, d)[:, None], row_of(label_all, d)[:, None])

        z_other, d_table = lax.optimization_barrier((z_other, d_table))
        dz_other = half_grad(other, z_other)
        dz_other = lax.ppermute(dz_other, 'fsdp', partner)
        found_other, found_own = place_rows(look_counts, look_codes.reshape(2, half, seq), e_half)
        found_other, z = lax.optimization_barrier((found_other, z))
        found_other = lax.ppermute(found_other, 'fsdp', partner)
        dz_own = half_grad(me, z)
        emb_rows = jnp.where(in_half[:, None], found_own[:, :dim], found_other[:, :dim]).reshape(1, seq, dim)

        de_all = lax.all_gather(d_emb.reshape(seq, dim), 'fsdp', axis=0, tiled=True)
        d_table, dz_own = lax.optimization_barrier((d_table, dz_own))
        d_table = add_rows(counts, codes, de_all, d_table)

        d_hidden, d_gain, d_bias = ln_vjp((dz_own + dz_other)[:, :dim])
        tail = jnp.concatenate([d_gain.reshape(n_dev, feat), d_bias.reshape(n_dev, feat), jnp.broadcast_to(loss_hit, (n_dev, 8))], axis=1)
        tail = jnp.sum(exchange(tail[:, None, :], n_dev, True, 4), axis=0)[0]
        mean_loss = loss_lse - tail[2 * feat]
        return (emb_rows, mean_loss, d_hidden.astype(BF16).reshape(1, seq, dim), d_table, tail[:feat], tail[feat:2 * feat])

    return jax.shard_map(device_step, mesh=mesh, in_specs=(batch_spec, batch_spec, batch_spec, act_spec, act_spec, batch_spec, vec_spec, vec_spec), out_specs=(act_spec, P(), act_spec, batch_spec, vec_spec, vec_spec), check_vma=False)
```

```python
import functools

import jax
import jax.numpy as jnp
from jax import lax
from jax.experimental import pallas as pl
from jax.experimental.pallas import tpu as pltpu
from jax.sharding import PartitionSpec as P

LN_EPSILON = 1e-5
F32 = jnp.float32
BF16 = jnp.bfloat16
VMEM_LIMIT = 60 * 1024 * 1024
CHUNKS = 2


def layer_norm(inputs, ln_gain, ln_bias):
    row_mean = jnp.mean(inputs, axis=-1, keepdims=True)
    centred = inputs - row_mean
    row_var = jnp.mean(centred * centred, axis=-1, keepdims=True)
    return centred * lax.rsqrt(row_var + LN_EPSILON) * ln_gain + ln_bias


def logits_body(*refs, sub, n_sub):
    e_ref, z_ref = refs[:2]
    lt_ref, zo_ref, m_ref, s_ref = refs[-4:]
    z = z_ref[...]
    zo_ref[...] = z
    m = s = None
    for j in range(n_sub):
        rows = slice(j * sub, (j + 1) * sub)
        l = lax.dot_general(e_ref[rows, :], z, (((1,), (1,)), ((), ())), preferred_element_type=F32)
        lt_ref[rows, :] = l
        m_here = jnp.max(l, axis=0, keepdims=True)
        if m is None:
            m_new = m_here
            s = jnp.sum(jnp.exp(l - m_new), axis=0, keepdims=True)
        else:
            m_new = jnp.maximum(m, m_here)
            s = s * jnp.exp(m - m_new) + jnp.sum(jnp.exp(l - m_new), axis=0, keepdims=True)
        m = m_new
    m_ref[...] = m
    s_ref[...] = s


def logits_pass(e, z, carry, chunk, total, pt=1024, sub=256):
    n_v, dim = e.shape
    n_p = z.shape[0]
    steps = n_p // pt
    first = chunk * steps
    in_specs = [pl.BlockSpec((n_v, dim), lambda i: (0, 0), pipeline_mode=pl.Buffered(1)), pl.BlockSpec((pt, dim), lambda i: (i, 0))]
    operands = [e, z]
    aliases = {}
    if carry is not None:
        in_specs += [pl.BlockSpec(memory_space=pl.ANY)] * 2
        operands += list(carry)
        aliases = {2: 0, 3: 1}
    return pl.pallas_call(
        functools.partial(logits_body, sub=sub, n_sub=n_v // sub),
        grid=(steps,),
        in_specs=in_specs,
        out_specs=[
            pl.BlockSpec((n_v, pt), lambda i: (0, i + first)),
            pl.BlockSpec((pt, dim), lambda i: (i + first, 0)),
            pl.BlockSpec((1, pt), lambda i: (0, i)),
            pl.BlockSpec((1, pt), lambda i: (0, i)),
        ],
        out_shape=[
            jax.ShapeDtypeStruct((n_v, total), F32),
            jax.ShapeDtypeStruct((total, dim), BF16),
            jax.ShapeDtypeStruct((1, n_p), F32),
            jax.ShapeDtypeStruct((1, n_p), F32),
        ],
        input_output_aliases=aliases,
        compiler_params=pltpu.CompilerParams(vmem_limit_bytes=VMEM_LIMIT, dimension_semantics=("arbitrary",)),
        cost_estimate=pl.CostEstimate(flops=2 * n_v * n_p * dim, bytes_accessed=4 * n_v * n_p + 2 * n_v * dim, transcendentals=n_v * n_p),
        name="logits_pass",
    )(*operands)


def table_grad_body(base_ref, lt_ref, z_ref, lse_ref, w_ref, y_ref, acc_ref, ll_ref, *, sub, n_sub):
    @pl.when(pl.program_id(0) == 0)
    def _():
        acc_ref[...] = jnp.zeros_like(acc_ref)

    lse = lse_ref[...]
    w = w_ref[...]
    y = y_ref[...] - base_ref[0]
    z = z_ref[...]
    row_ids = lax.broadcasted_iota(jnp.int32, (sub, z.shape[0]), 0)
    label_logit = jnp.zeros_like(lse)
    for j in range(n_sub):
        rows = slice(j * sub, (j + 1) * sub)
        l = lt_ref[rows, :]
        p = jnp.exp(l - lse)
        hit = row_ids == (y - j * sub)
        d = (w * jnp.where(hit, p - 1.0, p)).astype(BF16)
        label_logit = label_logit + jnp.sum(jnp.where(hit, l, 0.0), axis=0, keepdims=True)
        acc_ref[rows, :] += jnp.dot(d, z, preferred_element_type=F32)
    ll_ref[...] = label_logit


def table_grad(base, lt, z, lse, w, y, pt=1024, sub=512):
    n_v, n_p = lt.shape
    dim = z.shape[1]
    row = pl.BlockSpec((1, pt), lambda i, b: (0, i))
    return pl.pallas_call(
        functools.partial(table_grad_body, sub=sub, n_sub=n_v // sub),
        grid_spec=pltpu.PrefetchScalarGridSpec(
            num_scalar_prefetch=1,
            grid=(n_p // pt,),
            in_specs=[pl.BlockSpec((n_v, pt), lambda i, b: (0, i)), pl.BlockSpec((pt, dim), lambda i, b: (i, 0)), row, row, row],
            out_specs=[pl.BlockSpec((n_v, dim), lambda i, b: (0, 0), pipeline_mode=pl.Buffered(1)), row],
        ),
        out_shape=[jax.ShapeDtypeStruct((n_v, dim), F32), jax.ShapeDtypeStruct((1, n_p), F32)],
        compiler_params=pltpu.CompilerParams(vmem_limit_bytes=VMEM_LIMIT, dimension_semantics=("arbitrary",)),
        cost_estimate=pl.CostEstimate(flops=2 * n_v * n_p * dim, bytes_accessed=4 * n_v * n_p, transcendentals=n_v * n_p),
        name="table_grad",
    )(base, lt, z, lse, w, y)


def hidden_grad_body(base_ref, z_ref, e_ref, lse_ref, w_ref, y_ref, acc_ref, *, tp, n_tp, tv):
    i = pl.program_id(0)

    @pl.when(i == 0)
    def _():
        acc_ref[...] = jnp.zeros_like(acc_ref)

    e = e_ref[...]
    base = base_ref[0] + i * tv
    col_ids = lax.broadcasted_iota(jnp.int32, (tp, tv), 1)
    for j in range(n_tp):
        rows = slice(j * tp, (j + 1) * tp)
        l = lax.dot_general(z_ref[rows, :], e, (((1,), (1,)), ((), ())), preferred_element_type=F32)
        p = jnp.exp(l - lse_ref[rows, :])
        hit = col_ids == (y_ref[rows, :] - base)
        d = (w_ref[rows, :] * jnp.where(hit, p - 1.0, p)).astype(BF16)
        acc_ref[rows, :e.shape[1]] += jnp.dot(d, e, preferred_element_type=F32)


def hidden_grad(base, which, z, e, lse, w, y, tp=512, tv=768):
    n_v, dim = e.shape
    n_p = z.shape[0]
    wide = pl.cdiv(dim, 128) * 128
    col = pl.BlockSpec((n_p, 1), lambda i, b: (which, 0))
    return pl.pallas_call(
        functools.partial(hidden_grad_body, tp=tp, n_tp=n_p // tp, tv=tv),
        grid_spec=pltpu.PrefetchScalarGridSpec(
            num_scalar_prefetch=1,
            grid=(n_v // tv,),
            in_specs=[pl.BlockSpec((n_p, dim), lambda i, b: (0, 0)), pl.BlockSpec((tv, dim), lambda i, b: (i, 0)), col, col, col],
            out_specs=pl.BlockSpec((n_p, wide), lambda i, b: (0, 0), pipeline_mode=pl.Buffered(1)),
        ),
        out_shape=jax.ShapeDtypeStruct((n_p, wide), F32),
        compiler_params=pltpu.CompilerParams(vmem_limit_bytes=VMEM_LIMIT, dimension_semantics=("arbitrary",)),
        cost_estimate=pl.CostEstimate(flops=4 * n_v * n_p * dim, bytes_accessed=2 * n_v * dim, transcendentals=n_v * n_p),
        name="hidden_grad",
    )(base, z, e, lse, w, y)


def add_rows_body(count_ref, code_ref, de_ref, grad_ref, acc_ref, rows_ref):
    b = pl.program_id(0)

    @pl.when(b == 0)
    def _():
        pltpu.sync_copy(grad_ref, acc_ref)

    rows_ref[...] = de_ref[...].astype(F32)

    def step(k, carry):
        code = code_ref[0, 0, k]
        src = lax.shift_right_logical(code, 12)
        dst = lax.bitwise_and(code, 4095)
        acc_ref[pl.ds(dst, 1), :] += rows_ref[pl.ds(src, 1), :]
        return carry

    lax.fori_loop(0, count_ref[b], step, 0)


def add_rows(counts, codes, d_emb, grad):
    n_b, n_p = codes.shape
    n_v, dim = grad.shape
    whole = lambda b, c: (0, 0)
    return pl.pallas_call(
        add_rows_body,
        grid_spec=pltpu.PrefetchScalarGridSpec(
            num_scalar_prefetch=1,
            grid=(n_b,),
            in_specs=[
                pl.BlockSpec((1, 1, n_p), lambda b, c: (b, 0, 0), memory_space=pltpu.SMEM),
                pl.BlockSpec((n_p, dim), lambda b, c: (b, 0)),
                pl.BlockSpec(memory_space=pl.ANY),
            ],
            out_specs=pl.BlockSpec((n_v, dim), whole, pipeline_mode=pl.Buffered(1)),
            scratch_shapes=[pltpu.VMEM((n_p, dim), F32)],
        ),
        out_shape=jax.ShapeDtypeStruct((n_v, dim), F32),
        compiler_params=pltpu.CompilerParams(vmem_limit_bytes=VMEM_LIMIT, dimension_semantics=("arbitrary",)),
        cost_estimate=pl.CostEstimate(flops=10**10, bytes_accessed=2 * n_b * n_p * dim, transcendentals=0),
        name="add_rows",
    )(counts, codes.reshape(n_b, 1, n_p), d_emb, grad)


def place_rows_body(count_ref, code_ref, e_ref, first_ref, second_ref, wide_ref, rows_ref):
    b = pl.program_id(0)
    n_b = pl.num_programs(0)
    n_p = first_ref.shape[0]

    @pl.when(b == 0)
    def _():
        rows_ref[...] = jnp.zeros_like(rows_ref)

    wide_ref[...] = e_ref[...].astype(F32)

    for part in range(2):
        def step(k, carry):
            code = code_ref[0, part, k]
            dst = lax.shift_right_logical(code, 12) + part * n_p
            src = lax.bitwise_and(code, 4095)
            rows_ref[pl.ds(dst, 1), :] = wide_ref[pl.ds(src, 1), :]
            return carry

        lax.fori_loop(0, count_ref[part * n_b + b], step, 0)

    @pl.when(b == n_b - 1)
    def _():
        dim = rows_ref.shape[1]
        first_ref[:, :dim] = rows_ref[:n_p, :].astype(BF16)
        second_ref[:, :dim] = rows_ref[n_p:, :].astype(BF16)


def place_rows(counts, codes, e):
    _, n_b, n_p = codes.shape
    dim = e.shape[1]
    n_v = e.shape[0] // n_b
    wide = pl.cdiv(dim, 128) * 128
    out = pl.BlockSpec((n_p, wide), lambda b, c: (0, 0), pipeline_mode=pl.Buffered(1))
    return pl.pallas_call(
        place_rows_body,
        grid_spec=pltpu.PrefetchScalarGridSpec(
            num_scalar_prefetch=1,
            grid=(n_b,),
            in_specs=[
                pl.BlockSpec((1, 2, n_p), lambda b, c: (b, 0, 0), memory_space=pltpu.SMEM),
                pl.BlockSpec((n_v, dim), lambda b, c: (b, 0)),
            ],
            out_specs=[out, out],
            scratch_shapes=[pltpu.VMEM((n_v, dim), F32), pltpu.VMEM((2 * n_p, dim), F32)],
        ),
        out_shape=[jax.ShapeDtypeStruct((n_p, wide), BF16)] * 2,
        compiler_params=pltpu.CompilerParams(vmem_limit_bytes=VMEM_LIMIT, dimension_semantics=("arbitrary",)),
        cost_estimate=pl.CostEstimate(flops=10**10, bytes_accessed=2 * n_b * n_v * dim, transcendentals=0),
        name="place_rows",
    )(counts.reshape(-1), codes.transpose(1, 0, 2), e)


def exchange_body(x_ref, out_ref, send_sem, recv_sem, *, axis, n_dev, split):
    me = lax.axis_index(axis)
    barrier = pltpu.get_barrier_semaphore()
    for k in range(1, n_dev):
        pl.semaphore_signal(barrier, inc=1, device_id=(lax.rem(me + k, n_dev),), device_id_type=pl.DeviceIdType.MESH)
    pl.semaphore_wait(barrier, n_dev - 1)
    copies = []
    for k in range(1, n_dev):
        to = lax.rem(me + k, n_dev)
        copy = pltpu.make_async_remote_copy(
            src_ref=x_ref.at[to] if split else x_ref.at[0],
            dst_ref=out_ref.at[me],
            send_sem=send_sem.at[k - 1],
            recv_sem=recv_sem.at[k - 1],
            device_id=(to,),
            device_id_type=pl.DeviceIdType.MESH,
        )
        copy.start()
        copies.append(copy)
    out_ref[pl.ds(me, 1)] = x_ref[pl.ds(me, 1)] if split else x_ref[...]
    for copy in copies:
        copy.wait()


def exchange(x, n_dev, split, collective_id, axis='fsdp'):
    block = x.shape[1:]
    return pl.pallas_call(
        functools.partial(exchange_body, axis=axis, n_dev=n_dev, split=split),
        in_specs=[pl.BlockSpec(memory_space=pltpu.VMEM)],
        out_specs=pl.BlockSpec(memory_space=pltpu.VMEM),
        out_shape=jax.ShapeDtypeStruct((n_dev,) + block, x.dtype),
        scratch_shapes=[pltpu.SemaphoreType.DMA((n_dev - 1,)), pltpu.SemaphoreType.DMA((n_dev - 1,))],
        compiler_params=pltpu.CompilerParams(collective_id=collective_id, has_side_effects=True),
        cost_estimate=pl.CostEstimate(flops=4 * 10**9, bytes_accessed=0, transcendentals=0),
        name="exchange",
    )(x)


def solution(mesh):
    batch_spec = P('fsdp', None)
    act_spec = P('fsdp', None, None)
    vec_spec = P('fsdp')
    n_dev = mesh.shape['fsdp']
    half = n_dev // 2
    planes = [list(range(half)), list(range(half, n_dev))]
    partner = [(i, (i + half) % n_dev) for i in range(n_dev)]

    def device_step(tokens, labels, loss_mask, hidden, d_emb, table_shard, gain_shard, bias_shard):
        _, seq, dim = hidden.shape
        n_v = table_shard.shape[0]
        feat = gain_shard.shape[0]
        total = n_dev * seq
        part = seq // CHUNKS
        me = lax.axis_index('fsdp')
        other = lax.rem(me + half, n_dev)
        plane = me // half

        small = jnp.concatenate([tokens.reshape(-1).astype(F32), labels.reshape(-1).astype(F32), loss_mask.reshape(-1).astype(F32), gain_shard, bias_shard])
        small = jnp.pad(small, (0, 4 * 1024 - small.shape[0])).reshape(1, 32, 128)
        small = exchange(small, n_dev, False, 1).reshape(n_dev, 4 * 1024)
        tok_all = small[:, :seq].astype(jnp.int32)
        label_all = small[:, seq:2 * seq].astype(jnp.int32)
        mask_all = small[:, 2 * seq:3 * seq]
        ln_gain = small[:, 3 * seq:3 * seq + feat].reshape(-1)
        ln_bias = small[:, 3 * seq + feat:3 * seq + 2 * feat].reshape(-1)
        weight_all = mask_all / jnp.sum(mask_all)

        hid = hidden.reshape(seq, dim).astype(F32)
        normed, ln_vjp = jax.vjp(layer_norm, hid, ln_gain, ln_bias)
        z = normed.astype(BF16)

        def row_of(a, d):
            return lax.dynamic_index_in_dim(a, d, 0, keepdims=False)

        upto = (jnp.arange(seq)[:, None] <= jnp.arange(seq)[None, :]).astype(BF16)

        def pack(rel):
            hit = (rel >= 0) & (rel < n_v)
            rank = jnp.dot(hit.astype(BF16), upto, preferred_element_type=F32).astype(jnp.int32) - 1
            code = jnp.where(hit, jnp.arange(seq, dtype=jnp.int32)[None, :] * 4096 + rel, 0)
            slot = jnp.where(hit, rank, -1)
            codes = jnp.sum(jnp.where(slot[:, :, None] == jnp.arange(seq, dtype=jnp.int32)[None, None, :], code[:, :, None], 0), axis=1)
            return codes, jnp.sum(hit.astype(jnp.int32), axis=1)

        codes, counts = pack(tok_all - me * n_v)
        tok_own = row_of(tok_all, me)
        block_start = (plane * half + jnp.arange(half, dtype=jnp.int32)) * n_v
        look = jnp.stack([row_of(tok_all, other), tok_own])[:, None, :] - block_start[None, :, None]
        look_codes, look_counts = pack(look.reshape(2 * half, seq))
        in_half = (tok_own // (half * n_v)) == plane

        def by_chunk(a):
            return a.reshape(n_dev, CHUNKS, part).transpose(1, 0, 2).reshape(1, total)

        def columns(a):
            return jnp.concatenate([row_of(a, other), row_of(a, me)])[:, None]

        early = (codes, counts, look_codes, look_counts, by_chunk(weight_all), by_chunk(label_all), columns(weight_all), columns(label_all))

        carry = None
        maxes, sums, z_parts = [], [], []
        for c in range(CHUNKS):
            z_c = lax.all_gather(z[c * part:(c + 1) * part], 'fsdp', axis=0, tiled=True)
            if c == 0:
                z_c, early = lax.optimization_barrier((z_c, early))
                codes, counts, look_codes, look_counts, w_row, y_row, w_col, y_col = early
            lt, z_all, m_c, s_c = logits_pass(table_shard, z_c, carry, c, total)
            carry = (lt, z_all)
            maxes.append(m_c)
            sums.append(s_c)
            z_parts.append(lax.dynamic_slice_in_dim(z_c, other * part, part, 0))
        z_other = jnp.concatenate(z_parts, axis=0)

        def to_owner(parts):
            return jnp.stack([p.reshape(n_dev, part) for p in parts], axis=1).reshape(n_dev, seq // 128, 128)

        pairs = jnp.concatenate([to_owner(maxes), to_owner(sums)], axis=1)
        pairs = exchange(pairs, n_dev, True, 2)
        pair_max, pair_sum = pairs[:, :seq // 128], pairs[:, seq // 128:]
        row_max = jnp.max(pair_max, axis=0)
        row_sum = jnp.sum(pair_sum * jnp.exp(pair_max - row_max[None]), axis=0)
        lse_all = exchange((row_max + jnp.log(row_sum))[None], n_dev, False, 3).reshape(n_dev, seq)

        base = (me * n_v).astype(jnp.int32).reshape(1)
        d_table, label_logit = table_grad(base, lt, z_all, by_chunk(lse_all), w_row, y_row)
        loss_lse = jnp.sum(weight_all * lse_all)
        loss_hit = jnp.sum(w_row * label_logit)

        e_half = lax.all_gather(table_shard, 'fsdp', axis=0, tiled=True, axis_index_groups=planes)
        half_base = (plane * half * n_v).astype(jnp.int32)

        cols = columns(lse_all), w_col, y_col

        def half_grad(which, z_d):
            return hidden_grad(half_base.reshape(1), which, z_d, e_half, *cols)

        z_other, d_table = lax.optimization_barrier((z_other, d_table))
        dz_other = half_grad(0, z_other)
        dz_other = lax.ppermute(dz_other, 'fsdp', partner)
        found_other, found_own = place_rows(look_counts, look_codes.reshape(2, half, seq), e_half)
        found_other, z = lax.optimization_barrier((found_other, z))
        found_other = lax.ppermute(found_other, 'fsdp', partner)
        dz_own = half_grad(1, z)
        emb_rows = jnp.where(in_half[:, None], found_own[:, :dim], found_other[:, :dim]).reshape(1, seq, dim)

        de_all = lax.all_gather(d_emb.reshape(seq, dim), 'fsdp', axis=0, tiled=True)
        d_table, dz_own = lax.optimization_barrier((d_table, dz_own))
        d_table = add_rows(counts, codes, de_all, d_table)

        d_hidden, d_gain, d_bias = ln_vjp((dz_own + dz_other)[:, :dim])
        tail = jnp.concatenate([d_gain.reshape(n_dev, feat), d_bias.reshape(n_dev, feat), jnp.broadcast_to(loss_hit, (n_dev, 8))], axis=1)
        tail = jnp.sum(exchange(tail[:, None, :], n_dev, True, 4), axis=0)[0]
        mean_loss = loss_lse - tail[2 * feat]
        return (emb_rows, mean_loss, d_hidden.astype(BF16).reshape(1, seq, dim), d_table, tail[:feat], tail[feat:2 * feat])

    return jax.shard_map(device_step, mesh=mesh, in_specs=(batch_spec, batch_spec, batch_spec, act_spec, act_spec, batch_spec, vec_spec, vec_spec), out_specs=(act_spec, P(), act_spec, batch_spec, vec_spec, vec_spec), check_vma=False)
```

```python
import functools

import jax
import jax.numpy as jnp
from jax import lax
from jax.experimental import pallas as pl
from jax.experimental.pallas import tpu as pltpu
from jax.sharding import PartitionSpec as P

LN_EPSILON = 1e-5
F32 = jnp.float32
BF16 = jnp.bfloat16
VMEM_LIMIT = 60 * 1024 * 1024
CHUNKS = 2


def layer_norm(inputs, ln_gain, ln_bias):
    row_mean = jnp.mean(inputs, axis=-1, keepdims=True)
    centred = inputs - row_mean
    row_var = jnp.mean(centred * centred, axis=-1, keepdims=True)
    return centred * lax.rsqrt(row_var + LN_EPSILON) * ln_gain + ln_bias


def logits_body(*refs, sub, n_sub):
    e_ref, z_ref = refs[:2]
    lt_ref, zo_ref, m_ref, s_ref = refs[-4:]
    z = z_ref[...]
    zo_ref[...] = z
    m = s = None
    for j in range(n_sub):
        rows = slice(j * sub, (j + 1) * sub)
        l = lax.dot_general(e_ref[rows, :], z, (((1,), (1,)), ((), ())), preferred_element_type=F32)
        lt_ref[rows, :] = l
        m_here = jnp.max(l, axis=0, keepdims=True)
        if m is None:
            m_new = m_here
            s = jnp.sum(jnp.exp(l - m_new), axis=0, keepdims=True)
        else:
            m_new = jnp.maximum(m, m_here)
            s = s * jnp.exp(m - m_new) + jnp.sum(jnp.exp(l - m_new), axis=0, keepdims=True)
        m = m_new
    m_ref[...] = m
    s_ref[...] = s


def logits_pass(e, z, carry, chunk, total, pt=1024, sub=256):
    n_v, dim = e.shape
    n_p = z.shape[0]
    steps = n_p // pt
    first = chunk * steps
    in_specs = [pl.BlockSpec((n_v, dim), lambda i: (0, 0), pipeline_mode=pl.Buffered(1)), pl.BlockSpec((pt, dim), lambda i: (i, 0))]
    operands = [e, z]
    aliases = {}
    if carry is not None:
        in_specs += [pl.BlockSpec(memory_space=pl.ANY)] * 2
        operands += list(carry)
        aliases = {2: 0, 3: 1}
    return pl.pallas_call(
        functools.partial(logits_body, sub=sub, n_sub=n_v // sub),
        grid=(steps,),
        in_specs=in_specs,
        out_specs=[
            pl.BlockSpec((n_v, pt), lambda i: (0, i + first)),
            pl.BlockSpec((pt, dim), lambda i: (i + first, 0)),
            pl.BlockSpec((1, pt), lambda i: (0, i)),
            pl.BlockSpec((1, pt), lambda i: (0, i)),
        ],
        out_shape=[
            jax.ShapeDtypeStruct((n_v, total), F32),
            jax.ShapeDtypeStruct((total, dim), BF16),
            jax.ShapeDtypeStruct((1, n_p), F32),
            jax.ShapeDtypeStruct((1, n_p), F32),
        ],
        input_output_aliases=aliases,
        compiler_params=pltpu.CompilerParams(vmem_limit_bytes=VMEM_LIMIT, dimension_semantics=("arbitrary",)),
        cost_estimate=pl.CostEstimate(flops=2 * n_v * n_p * dim, bytes_accessed=4 * n_v * n_p + 2 * n_v * dim, transcendentals=n_v * n_p),
        name="logits_pass",
    )(*operands)


def table_grad_body(base_ref, lt_ref, z_ref, lse_ref, w_ref, y_ref, acc_ref, ll_ref, *, sub, n_sub):
    @pl.when(pl.program_id(0) == 0)
    def _():
        acc_ref[...] = jnp.zeros_like(acc_ref)

    lse = lse_ref[...]
    w = w_ref[...]
    y = y_ref[...] - base_ref[0]
    z = z_ref[...]
    row_ids = lax.broadcasted_iota(jnp.int32, (sub, z.shape[0]), 0)
    label_logit = jnp.zeros_like(lse)
    for j in range(n_sub):
        rows = slice(j * sub, (j + 1) * sub)
        l = lt_ref[rows, :]
        p = jnp.exp(l - lse)
        hit = row_ids == (y - j * sub)
        d = (w * jnp.where(hit, p - 1.0, p)).astype(BF16)
        label_logit = label_logit + jnp.sum(jnp.where(hit, l, 0.0), axis=0, keepdims=True)
        acc_ref[rows, :] += jnp.dot(d, z, preferred_element_type=F32)
    ll_ref[...] = label_logit


def table_grad(base, lt, z, lse, w, y, pt=1024, sub=256):
    n_v, n_p = lt.shape
    dim = z.shape[1]
    row = pl.BlockSpec((1, pt), lambda i, b: (0, i))
    return pl.pallas_call(
        functools.partial(table_grad_body, sub=sub, n_sub=n_v // sub),
        grid_spec=pltpu.PrefetchScalarGridSpec(
            num_scalar_prefetch=1,
            grid=(n_p // pt,),
            in_specs=[pl.BlockSpec((n_v, pt), lambda i, b: (0, i)), pl.BlockSpec((pt, dim), lambda i, b: (i, 0)), row, row, row],
            out_specs=[pl.BlockSpec((n_v, dim), lambda i, b: (0, 0), pipeline_mode=pl.Buffered(1)), row],
        ),
        out_shape=[jax.ShapeDtypeStruct((n_v, dim), F32), jax.ShapeDtypeStruct((1, n_p), F32)],
        compiler_params=pltpu.CompilerParams(vmem_limit_bytes=VMEM_LIMIT, dimension_semantics=("arbitrary",)),
        cost_estimate=pl.CostEstimate(flops=2 * n_v * n_p * dim, bytes_accessed=4 * n_v * n_p, transcendentals=n_v * n_p),
        name="table_grad",
    )(base, lt, z, lse, w, y)


def hidden_grad_body(base_ref, z_ref, e_ref, lse_ref, w_ref, y_ref, acc_ref, *, tp, n_tp, tv):
    i = pl.program_id(0)

    @pl.when(i == 0)
    def _():
        acc_ref[...] = jnp.zeros_like(acc_ref)

    e = e_ref[...]
    base = base_ref[0] + i * tv
    col_ids = lax.broadcasted_iota(jnp.int32, (tp, tv), 1)
    for j in range(n_tp):
        rows = slice(j * tp, (j + 1) * tp)
        l = lax.dot_general(z_ref[rows, :], e, (((1,), (1,)), ((), ())), preferred_element_type=F32)
        p = jnp.exp(l - lse_ref[rows, :])
        hit = col_ids == (y_ref[rows, :] - base)
        d = (w_ref[rows, :] * jnp.where(hit, p - 1.0, p)).astype(BF16)
        acc_ref[rows, :e.shape[1]] += jnp.dot(d, e, preferred_element_type=F32)


def hidden_grad(base, which, z, e, lse, w, y, tp=512, tv=768):
    n_v, dim = e.shape
    n_p = z.shape[0]
    wide = pl.cdiv(dim, 128) * 128
    col = pl.BlockSpec((n_p, 1), lambda i, b: (which, 0))
    return pl.pallas_call(
        functools.partial(hidden_grad_body, tp=tp, n_tp=n_p // tp, tv=tv),
        grid_spec=pltpu.PrefetchScalarGridSpec(
            num_scalar_prefetch=1,
            grid=(n_v // tv,),
            in_specs=[pl.BlockSpec((n_p, dim), lambda i, b: (0, 0)), pl.BlockSpec((tv, dim), lambda i, b: (i, 0)), col, col, col],
            out_specs=pl.BlockSpec((n_p, wide), lambda i, b: (0, 0), pipeline_mode=pl.Buffered(1)),
        ),
        out_shape=jax.ShapeDtypeStruct((n_p, wide), F32),
        compiler_params=pltpu.CompilerParams(vmem_limit_bytes=VMEM_LIMIT, dimension_semantics=("arbitrary",)),
        cost_estimate=pl.CostEstimate(flops=4 * n_v * n_p * dim, bytes_accessed=2 * n_v * dim, transcendentals=n_v * n_p),
        name="hidden_grad",
    )(base, z, e, lse, w, y)


def add_rows_body(count_ref, code_ref, de_ref, grad_ref, acc_ref, rows_ref):
    b = pl.program_id(0)

    @pl.when(b == 0)
    def _():
        pltpu.sync_copy(grad_ref, acc_ref)

    rows_ref[...] = de_ref[...].astype(F32)

    def step(k, carry):
        code = code_ref[0, 0, k]
        src = lax.shift_right_logical(code, 12)
        dst = lax.bitwise_and(code, 4095)
        acc_ref[pl.ds(dst, 1), :] += rows_ref[pl.ds(src, 1), :]
        return carry

    lax.fori_loop(0, count_ref[b], step, 0)


def add_rows(counts, codes, d_emb, grad):
    n_b, n_p = codes.shape
    n_v, dim = grad.shape
    whole = lambda b, c: (0, 0)
    return pl.pallas_call(
        add_rows_body,
        grid_spec=pltpu.PrefetchScalarGridSpec(
            num_scalar_prefetch=1,
            grid=(n_b,),
            in_specs=[
                pl.BlockSpec((1, 1, n_p), lambda b, c: (b, 0, 0), memory_space=pltpu.SMEM),
                pl.BlockSpec((n_p, dim), lambda b, c: (b, 0)),
                pl.BlockSpec(memory_space=pl.ANY),
            ],
            out_specs=pl.BlockSpec((n_v, dim), whole, pipeline_mode=pl.Buffered(1)),
            scratch_shapes=[pltpu.VMEM((n_p, dim), F32)],
        ),
        out_shape=jax.ShapeDtypeStruct((n_v, dim), F32),
        compiler_params=pltpu.CompilerParams(vmem_limit_bytes=VMEM_LIMIT, dimension_semantics=("arbitrary",)),
        cost_estimate=pl.CostEstimate(flops=10**10, bytes_accessed=2 * n_b * n_p * dim, transcendentals=0),
        name="add_rows",
    )(counts, codes.reshape(n_b, 1, n_p), d_emb, grad)


def place_rows_body(count_ref, code_ref, e_ref, first_ref, second_ref, wide_ref, rows_ref):
    b = pl.program_id(0)
    n_b = pl.num_programs(0)
    n_p = first_ref.shape[0]

    @pl.when(b == 0)
    def _():
        rows_ref[...] = jnp.zeros_like(rows_ref)

    wide_ref[...] = e_ref[...].astype(F32)

    for part in range(2):
        def step(k, carry):
            code = code_ref[0, part, k]
            dst = lax.shift_right_logical(code, 12) + part * n_p
            src = lax.bitwise_and(code, 4095)
            rows_ref[pl.ds(dst, 1), :] = wide_ref[pl.ds(src, 1), :]
            return carry

        lax.fori_loop(0, count_ref[part * n_b + b], step, 0)

    @pl.when(b == n_b - 1)
    def _():
        dim = rows_ref.shape[1]
        first_ref[:, :dim] = rows_ref[:n_p, :].astype(BF16)
        second_ref[:, :dim] = rows_ref[n_p:, :].astype(BF16)


def place_rows(counts, codes, e):
    _, n_b, n_p = codes.shape
    dim = e.shape[1]
    n_v = e.shape[0] // n_b
    wide = pl.cdiv(dim, 128) * 128
    out = pl.BlockSpec((n_p, wide), lambda b, c: (0, 0), pipeline_mode=pl.Buffered(1))
    return pl.pallas_call(
        place_rows_body,
        grid_spec=pltpu.PrefetchScalarGridSpec(
            num_scalar_prefetch=1,
            grid=(n_b,),
            in_specs=[
                pl.BlockSpec((1, 2, n_p), lambda b, c: (b, 0, 0), memory_space=pltpu.SMEM),
                pl.BlockSpec((n_v, dim), lambda b, c: (b, 0)),
            ],
            out_specs=[out, out],
            scratch_shapes=[pltpu.VMEM((n_v, dim), F32), pltpu.VMEM((2 * n_p, dim), F32)],
        ),
        out_shape=[jax.ShapeDtypeStruct((n_p, wide), BF16)] * 2,
        compiler_params=pltpu.CompilerParams(vmem_limit_bytes=VMEM_LIMIT, dimension_semantics=("arbitrary",)),
        cost_estimate=pl.CostEstimate(flops=10**10, bytes_accessed=2 * n_b * n_v * dim, transcendentals=0),
        name="place_rows",
    )(counts.reshape(-1), codes.transpose(1, 0, 2), e)


def exchange_body(x_ref, out_ref, send_sem, recv_sem, *, axis, n_dev, split):
    me = lax.axis_index(axis)
    barrier = pltpu.get_barrier_semaphore()
    for k in range(1, n_dev):
        pl.semaphore_signal(barrier, inc=1, device_id=(lax.rem(me + k, n_dev),), device_id_type=pl.DeviceIdType.MESH)
    pl.semaphore_wait(barrier, n_dev - 1)
    copies = []
    for k in range(1, n_dev):
        to = lax.rem(me + k, n_dev)
        copy = pltpu.make_async_remote_copy(
            src_ref=x_ref.at[to] if split else x_ref.at[0],
            dst_ref=out_ref.at[me],
            send_sem=send_sem.at[k - 1],
            recv_sem=recv_sem.at[k - 1],
            device_id=(to,),
            device_id_type=pl.DeviceIdType.MESH,
        )
        copy.start()
        copies.append(copy)
    out_ref[pl.ds(me, 1)] = x_ref[pl.ds(me, 1)] if split else x_ref[...]
    for copy in copies:
        copy.wait()


def exchange(x, n_dev, split, collective_id, axis='fsdp'):
    block = x.shape[1:]
    return pl.pallas_call(
        functools.partial(exchange_body, axis=axis, n_dev=n_dev, split=split),
        in_specs=[pl.BlockSpec(memory_space=pltpu.VMEM)],
        out_specs=pl.BlockSpec(memory_space=pltpu.VMEM),
        out_shape=jax.ShapeDtypeStruct((n_dev,) + block, x.dtype),
        scratch_shapes=[pltpu.SemaphoreType.DMA((n_dev - 1,)), pltpu.SemaphoreType.DMA((n_dev - 1,))],
        compiler_params=pltpu.CompilerParams(collective_id=collective_id, has_side_effects=True),
        cost_estimate=pl.CostEstimate(flops=4 * 10**9, bytes_accessed=0, transcendentals=0),
        name="exchange",
    )(x)


def solution(mesh):
    batch_spec = P('fsdp', None)
    act_spec = P('fsdp', None, None)
    vec_spec = P('fsdp')
    n_dev = mesh.shape['fsdp']
    half = n_dev // 2
    planes = [list(range(half)), list(range(half, n_dev))]
    partner = [(i, (i + half) % n_dev) for i in range(n_dev)]

    def device_step(tokens, labels, loss_mask, hidden, d_emb, table_shard, gain_shard, bias_shard):
        _, seq, dim = hidden.shape
        n_v = table_shard.shape[0]
        feat = gain_shard.shape[0]
        total = n_dev * seq
        part = seq // CHUNKS
        me = lax.axis_index('fsdp')
        other = lax.rem(me + half, n_dev)
        plane = me // half

        small = jnp.concatenate([tokens.reshape(-1).astype(F32), labels.reshape(-1).astype(F32), loss_mask.reshape(-1).astype(F32), gain_shard, bias_shard])
        small = jnp.pad(small, (0, 4 * 1024 - small.shape[0])).reshape(1, 32, 128)
        small = exchange(small, n_dev, False, 1).reshape(n_dev, 4 * 1024)
        tok_all = small[:, :seq].astype(jnp.int32)
        label_all = small[:, seq:2 * seq].astype(jnp.int32)
        mask_all = small[:, 2 * seq:3 * seq]
        ln_gain = small[:, 3 * seq:3 * seq + feat].reshape(-1)
        ln_bias = small[:, 3 * seq + feat:3 * seq + 2 * feat].reshape(-1)
        weight_all = mask_all / jnp.sum(mask_all)

        hid = hidden.reshape(seq, dim).astype(F32)
        normed, ln_vjp = jax.vjp(layer_norm, hid, ln_gain, ln_bias)
        z = normed.astype(BF16)

        def row_of(a, d):
            return lax.dynamic_index_in_dim(a, d, 0, keepdims=False)

        upto = (jnp.arange(seq)[:, None] <= jnp.arange(seq)[None, :]).astype(BF16)

        def pack(rel):
            hit = (rel >= 0) & (rel < n_v)
            rank = jnp.dot(hit.astype(BF16), upto, preferred_element_type=F32).astype(jnp.int32) - 1
            code = jnp.where(hit, jnp.arange(seq, dtype=jnp.int32)[None, :] * 4096 + rel, 0)
            slot = jnp.where(hit, rank, -1)
            codes = jnp.sum(jnp.where(slot[:, :, None] == jnp.arange(seq, dtype=jnp.int32)[None, None, :], code[:, :, None], 0), axis=1)
            return codes, jnp.sum(hit.astype(jnp.int32), axis=1)

        codes, counts = pack(tok_all - me * n_v)
        tok_own = row_of(tok_all, me)
        block_start = (plane * half + jnp.arange(half, dtype=jnp.int32)) * n_v
        look = jnp.stack([row_of(tok_all, other), tok_own])[:, None, :] - block_start[None, :, None]
        look_codes, look_counts = pack(look.reshape(2 * half, seq))
        in_half = (tok_own // (half * n_v)) == plane

        def by_chunk(a):
            return a.reshape(n_dev, CHUNKS, part).transpose(1, 0, 2).reshape(1, total)

        def columns(a):
            return jnp.concatenate([row_of(a, other), row_of(a, me)])[:, None]

        early = (codes, counts, look_codes, look_counts, by_chunk(weight_all), by_chunk(label_all), columns(weight_all), columns(label_all))

        carry = None
        maxes, sums, z_parts = [], [], []
        for c in range(CHUNKS):
            z_c = lax.all_gather(z[c * part:(c + 1) * part], 'fsdp', axis=0, tiled=True)
            if c == 0:
                z_c, early = lax.optimization_barrier((z_c, early))
                codes, counts, look_codes, look_counts, w_row, y_row, w_col, y_col = early
            lt, z_all, m_c, s_c = logits_pass(table_shard, z_c, carry, c, total)
            carry = (lt, z_all)
            maxes.append(m_c)
            sums.append(s_c)
            z_parts.append(lax.dynamic_slice_in_dim(z_c, other * part, part, 0))
        z_other = jnp.concatenate(z_parts, axis=0)

        def to_owner(parts):
            return jnp.stack([p.reshape(n_dev, part) for p in parts], axis=1).reshape(n_dev, seq // 128, 128)

        pairs = jnp.concatenate([to_owner(maxes), to_owner(sums)], axis=1)
        pairs = exchange(pairs, n_dev, True, 2)
        pair_max, pair_sum = pairs[:, :seq // 128], pairs[:, seq // 128:]
        row_max = jnp.max(pair_max, axis=0)
        row_sum = jnp.sum(pair_sum * jnp.exp(pair_max - row_max[None]), axis=0)
        lse_all = exchange((row_max + jnp.log(row_sum))[None], n_dev, False, 3).reshape(n_dev, seq)

        base = (me * n_v).astype(jnp.int32).reshape(1)
        d_table, label_logit = table_grad(base, lt, z_all, by_chunk(lse_all), w_row, y_row)
        loss_lse = jnp.sum(weight_all * lse_all)
        loss_hit = jnp.sum(w_row * label_logit)

        e_half = lax.all_gather(table_shard, 'fsdp', axis=0, tiled=True, axis_index_groups=planes)
        half_base = (plane * half * n_v).astype(jnp.int32)

        cols = columns(lse_all), w_col, y_col

        def half_grad(which, z_d):
            return hidden_grad(half_base.reshape(1), which, z_d, e_half, *cols)

        z_other, d_table = lax.optimization_barrier((z_other, d_table))
        dz_other = half_grad(0, z_other)
        dz_other = lax.ppermute(dz_other, 'fsdp', partner)
        found_other, found_own = place_rows(look_counts, look_codes.reshape(2, half, seq), e_half)
        found_other, z = lax.optimization_barrier((found_other, z))
        found_other = lax.ppermute(found_other, 'fsdp', partner)
        dz_own = half_grad(1, z)
        emb_rows = jnp.where(in_half[:, None], found_own[:, :dim], found_other[:, :dim]).reshape(1, seq, dim)

        de_all = lax.all_gather(d_emb.reshape(seq, dim), 'fsdp', axis=0, tiled=True)
        d_table, dz_own = lax.optimization_barrier((d_table, dz_own))
        d_table = add_rows(counts, codes, de_all, d_table)

        d_hidden, d_gain, d_bias = ln_vjp((dz_own + dz_other)[:, :dim])
        tail = jnp.concatenate([d_gain.reshape(n_dev, feat), d_bias.reshape(n_dev, feat), jnp.broadcast_to(loss_hit, (n_dev, 8))], axis=1)
        tail = jnp.sum(exchange(tail[:, None, :], n_dev, True, 4), axis=0)[0]
        mean_loss = loss_lse - tail[2 * feat]
        return (emb_rows, mean_loss, d_hidden.astype(BF16).reshape(1, seq, dim), d_table, tail[:feat], tail[feat:2 * feat])

    return jax.shard_map(device_step, mesh=mesh, in_specs=(batch_spec, batch_spec, batch_spec, act_spec, act_spec, batch_spec, vec_spec, vec_spec), out_specs=(act_spec, P(), act_spec, batch_spec, vec_spec, vec_spec), check_vma=False)
```
